16 devices in a mesh: dp: 4 (over z, y), sp: 4 (over x, core).
Axes of the slice: x: 2, y: 2, z: 2, core: 2. Of those that a mesh axis runs over, the one named last changes fastest.
Arguments:
- image_in: bfloat16 [16, 256, 1536], P('dp', 'sp'), parts along dimension 0
- text_in: bfloat16 [16, 333, 1536], P('dp'), parts along dimension 0
- cond_vec: bfloat16 [16, 1536], P('dp'), parts along dimension 0
- w_ada: bfloat16 [2, 1536, 4608], replicated
- b_ada: float32 [2, 4608], replicated
- w_qkv: bfloat16 [2, 1536, 4608], replicated
- b_qkv: float32 [2, 4608], replicated
- qk_gain: float32 [2, 2, 64], replicated
- w_out: bfloat16 [2, 1536, 1536], replicated
- b_out: float32 [2, 1536], replicated
- image_cot: bfloat16 [16, 256, 1536], P('dp', 'sp'), parts along dimension 0
- text_cot: bfloat16 [16, 333, 1536], P('dp'), parts along dimension 0
Outputs:
- output 1: bfloat16 [16, 256, 1536], P('dp', 'sp'), parts along dimension 0
- output 2: bfloat16 [16, 333, 1536], P('dp'), parts along dimension 0
- output 3: bfloat16 [16, 256, 1536], P('dp', 'sp'), parts along dimension 0
- output 4: bfloat16 [16, 333, 1536], P('dp'), parts along dimension 0
- output 5: float32 [16, 1536], P('dp'), parts along dimension 0
- output 6: float32 [8, 1536, 4608], P('dp'), parts along dimension 0
- output 7: float32 [8, 4608], P('dp'), parts along dimension 0
- output 8: float32 [8, 1536, 4608], P('dp'), parts along dimension 0
- output 9: float32 [8, 4608], P('dp'), parts along dimension 0
- output 10: float32 [8, 2, 64], P('dp'), parts along dimension 0
- output 11: float32 [8, 1536, 1536], P('dp'), parts along dimension 0
- output 12: float32 [8, 1536], P('dp'), parts along dimension 0
There are 4 independent parts. The reference program is written for one: setup_inputs(seed, part) draws one part's arguments, and reference() takes and returns one part's arrays. A program takes and returns all parts, laid end to end along the dimension named above; an argument that names none is the same for every part.
All inputs are finite; a program needn't handle non-finite values.
Results may differ from the reference program's by a relative error of at most 0.0130064.
Values are sent between devices in bfloat16 or wider.
A program may use at most 1 GiB of HBM per device.

```python
import math
import jax
import jax.numpy as jnp
from jax import lax

BATCH_SIZE = 4
IMG_TOKENS = 256
CTX_TOKENS = 333
MODEL_WIDTH = 1536
NUM_HEADS = 24
HEAD_DIM = 64
NORM_EPS = 1e-6
QUERY_ROWS = math.gcd(IMG_TOKENS, 512)
ATT_SCALE = HEAD_DIM ** -0.5


def setup_inputs(seed: int = 0, part: int = 0) -> dict:
    shared_keys = jax.random.split(jax.random.key(seed), 8)
    part_keys = jax.random.split(jax.random.fold_in(jax.random.key(seed + 1), part), 6)
    d_model = MODEL_WIDTH
    fan_scale = d_model ** -0.5
    image_in = jax.random.normal(part_keys[0], (BATCH_SIZE, IMG_TOKENS, d_model), jnp.float32)
    text_pattern = 2.0 * jax.random.normal(part_keys[1], (1, 1, d_model), jnp.float32)
    text_in = text_pattern + 0.7 * jax.random.normal(part_keys[2], (BATCH_SIZE, CTX_TOKENS, d_model), jnp.float32)
    cond_vec = jax.random.normal(part_keys[3], (BATCH_SIZE, d_model), jnp.float32)
    w_ada = 0.5 * fan_scale * jax.random.normal(shared_keys[0], (2, d_model, 3 * d_model), jnp.float32)
    b_ada = 0.5 * jax.random.normal(shared_keys[1], (2, 3 * d_model), jnp.float32)
    w_qkv = fan_scale * jax.random.normal(shared_keys[2], (2, d_model, 3 * d_model), jnp.float32)
    b_qkv = 0.3 * jax.random.normal(shared_keys[3], (2, 3 * d_model), jnp.float32)
    qk_gain = jax.random.uniform(shared_keys[4], (2, 2, HEAD_DIM), jnp.float32, 0.4, 2.0)
    w_out = fan_scale * jax.random.normal(shared_keys[5], (2, d_model, d_model), jnp.float32)
    b_out = 0.3 * jax.random.normal(shared_keys[6], (2, d_model), jnp.float32)
    image_cot = jax.random.normal(part_keys[4], (BATCH_SIZE, IMG_TOKENS, d_model), jnp.float32)
    text_cot = jax.random.normal(part_keys[5], (BATCH_SIZE, CTX_TOKENS, d_model), jnp.float32)
    return {'image_in': image_in.astype(jnp.bfloat16), 'text_in': text_in.astype(jnp.bfloat16), 'cond_vec': cond_vec.astype(jnp.bfloat16), 'w_ada': w_ada.astype(jnp.bfloat16), 'b_ada': b_ada, 'w_qkv': w_qkv.astype(jnp.bfloat16), 'b_qkv': b_qkv, 'qk_gain': qk_gain, 'w_out': w_out.astype(jnp.bfloat16), 'b_out': b_out, 'image_cot': image_cot.astype(jnp.bfloat16), 'text_cot': text_cot.astype(jnp.bfloat16)}


def norm_modulate(tokens, shift_vec, scale_vec):
    avg_val = jnp.mean(tokens, axis=-1, keepdims=True)
    centred = tokens - avg_val
    var_val = jnp.mean(centred * centred, axis=-1, keepdims=True)
    normed = centred * lax.rsqrt(var_val + NORM_EPS)
    return (normed * (1.0 + scale_vec[:, None, :]) + shift_vec[:, None, :]).astype(jnp.bfloat16)


def head_rms(raw_vals, gain_vec):
    inv_rms = lax.rsqrt(jnp.mean(raw_vals * raw_vals, axis=-1, keepdims=True) + NORM_EPS)
    return (raw_vals * inv_rms * gain_vec).astype(jnp.bfloat16)


def branch_qkv(tokens, cond_mod, w_proj, b_proj, gain_pair):
    n_tok = tokens.shape[1]
    hidden = norm_modulate(tokens, cond_mod[:, :MODEL_WIDTH], cond_mod[:, MODEL_WIDTH:2 * MODEL_WIDTH])
    proj_all = jnp.einsum('btd,de->bte', hidden.astype(jnp.float32), w_proj) + b_proj
    proj_all = proj_all.reshape(BATCH_SIZE, n_tok, 3, NUM_HEADS, HEAD_DIM)
    return head_rms(proj_all[:, :, 0], gain_pair[0]), head_rms(proj_all[:, :, 1], gain_pair[1]), proj_all[:, :, 2].astype(jnp.bfloat16)


def attend_rows(q_rows, key_rows, val_rows):
    scores = jnp.einsum('brf,bsf->brs', q_rows.astype(jnp.float32), key_rows.astype(jnp.float32)) * ATT_SCALE
    prob_mat = jax.nn.softmax(scores, axis=-1).astype(jnp.bfloat16)
    return jnp.einsum('brs,bsf->brf', prob_mat.astype(jnp.float32), val_rows.astype(jnp.float32)).astype(jnp.bfloat16)


def one_head(head_arrays):
    q_head, k_head, v_head = head_arrays
    block_fn = jax.checkpoint(attend_rows)
    out_txt = block_fn(q_head[:, :CTX_TOKENS], k_head, v_head)
    q_blocks = q_head[:, CTX_TOKENS:].reshape(BATCH_SIZE, IMG_TOKENS // QUERY_ROWS, QUERY_ROWS, HEAD_DIM).swapaxes(0, 1)
    out_blocks = lax.map(lambda q_block: block_fn(q_block, k_head, v_head), q_blocks)
    out_img = out_blocks.swapaxes(0, 1).reshape(BATCH_SIZE, IMG_TOKENS, HEAD_DIM)
    return jnp.concatenate([out_txt, out_img], axis=1)


def joint_attention(queries, keys_all, vals_all):
    head_major = (jnp.transpose(queries, (2, 0, 1, 3)), jnp.transpose(keys_all, (2, 0, 1, 3)), jnp.transpose(vals_all, (2, 0, 1, 3)))
    outs_all = lax.map(jax.checkpoint(one_head), head_major)
    return jnp.transpose(outs_all, (1, 2, 0, 3))


def forward(image_in, text_in, cond_vec, w_ada, b_ada, w_qkv, b_qkv, qk_gain, w_out, b_out):
    cond_act = jax.nn.silu(cond_vec).astype(jnp.bfloat16).astype(jnp.float32)
    cond_mod = jnp.einsum('bd,sde->sbe', cond_act, w_ada) + b_ada[:, None, :]
    q_img, k_img, v_img = branch_qkv(image_in, cond_mod[0], w_qkv[0], b_qkv[0], qk_gain[0])
    q_txt, k_txt, v_txt = branch_qkv(text_in, cond_mod[1], w_qkv[1], b_qkv[1], qk_gain[1])
    joint_out = joint_attention(jnp.concatenate([q_txt, q_img], axis=1), jnp.concatenate([k_txt, k_img], axis=1), jnp.concatenate([v_txt, v_img], axis=1))
    out_txt = joint_out[:, :CTX_TOKENS].reshape(BATCH_SIZE, CTX_TOKENS, MODEL_WIDTH).astype(jnp.float32)
    out_img = joint_out[:, CTX_TOKENS:].reshape(BATCH_SIZE, IMG_TOKENS, MODEL_WIDTH).astype(jnp.float32)
    gate_img = cond_mod[0][:, None, 2 * MODEL_WIDTH:]
    gate_txt = cond_mod[1][:, None, 2 * MODEL_WIDTH:]
    new_img = image_in + gate_img * (jnp.einsum('btd,de->bte', out_img, w_out[0]) + b_out[0])
    new_txt = text_in + gate_txt * (jnp.einsum('btd,de->bte', out_txt, w_out[1]) + b_out[1])
    return new_img.astype(jnp.bfloat16), new_txt.astype(jnp.bfloat16)


def reference(image_in, text_in, cond_vec, w_ada, b_ada, w_qkv, b_qkv, qk_gain, w_out, b_out, image_cot, text_cot):
    outs_pair, pullback = jax.vjp(forward, image_in.astype(jnp.float32), text_in.astype(jnp.float32), cond_vec.astype(jnp.float32), w_ada.astype(jnp.float32), b_ada, w_qkv.astype(jnp.float32), b_qkv, qk_gain, w_out.astype(jnp.float32), b_out)
    grads = pullback((image_cot, text_cot))
    return (outs_pair[0], outs_pair[1], grads[0].astype(jnp.bfloat16), grads[1].astype(jnp.bfloat16), grads[2], grads[3], grads[4], grads[5], grads[6], grads[7], grads[8], grads[9])
```

```python
import functools
import math
import jax
import jax.numpy as jnp
from jax import lax
from jax.experimental import pallas as pl
from jax.experimental.pallas import tpu as pltpu
from jax.sharding import PartitionSpec as P

NORM_EPS = 1e-6
F32 = jnp.float32
BF16 = jnp.bfloat16
NN = (((1,), (0,)), ((), ()))
NT = (((1,), (1,)), ((), ()))
TN = (((0,), (0,)), ((), ()))


def dot(lhs, rhs, dims=NN):
    return lax.dot_general(lhs, rhs, dims, preferred_element_type=F32)


def round_up(num, mult):
    return -(-num // mult) * mult


def stats(tokens):
    avg_val = jnp.mean(tokens, axis=-1, keepdims=True)
    centred = tokens - avg_val
    var_val = jnp.mean(centred * centred, axis=-1, keepdims=True)
    inv_std = lax.rsqrt(var_val + NORM_EPS)
    return centred * inv_std, inv_std


def prologue(tok_ref, cot_ref, mod_ref, hid_ref, dy_ref, chunk):
    @pl.loop(0, tok_ref.shape[0] // chunk)
    def _(step):
        rows = pl.ds(pl.multiple_of(step * chunk, chunk), chunk)
        normed, _ = stats(tok_ref[rows].astype(F32))
        hid_ref[rows] = (normed * (1.0 + mod_ref[1:2]) + mod_ref[0:1]).astype(BF16)
        dy_ref[rows] = (cot_ref[rows].astype(F32) * mod_ref[2:3]).astype(BF16)


def epilogue(tok_ref, cot_ref, mod_ref, bias, y_ref, acc_ref, new_ref, grad_ref, sums_ref, base, chunk):
    sums_ref[base:base + 4] = jnp.zeros((4, sums_ref.shape[1]), F32)

    @pl.loop(0, tok_ref.shape[0] // chunk)
    def _(step):
        rows = pl.ds(pl.multiple_of(step * chunk, chunk), chunk)
        tokens, cot = tok_ref[rows].astype(F32), cot_ref[rows].astype(F32)
        gate = mod_ref[2:3]
        y_out = y_ref[rows] + bias
        new_ref[rows] = (tokens + gate * y_out).astype(BF16)
        normed, inv_std = stats(tokens)
        d_hid = acc_ref[rows].astype(BF16).astype(F32)
        d_normed = d_hid * (1.0 + mod_ref[1:2])
        mean_d = jnp.mean(d_normed, axis=-1, keepdims=True)
        mean_dn = jnp.mean(d_normed * normed, axis=-1, keepdims=True)
        grad_ref[rows] = (cot + inv_std * (d_normed - mean_d - normed * mean_dn)).astype(BF16)
        sums_ref[base:base + 1] += jnp.sum(d_hid, axis=0, keepdims=True)
        sums_ref[base + 1:base + 2] += jnp.sum(d_hid * normed, axis=0, keepdims=True)
        sums_ref[base + 2:base + 3] += jnp.sum(cot * y_out, axis=0, keepdims=True)
        sums_ref[base + 3:base + 4] += jnp.sum(cot * gate, axis=0, keepdims=True)


def block_kernel(n_keys, heads, tok_i_ref, cot_i_ref, tok_t_ref, cot_t_ref, mod_ref, bo_ref, wq_ref, wk_ref, wv_ref, bq_ref, bk_ref, bv_ref, gain_ref, wo_ref,
                 hid_i_ref, hid_t_ref, dy_i_ref, dy_t_ref, o_i_ref, o_t_ref, dp_i_ref, dp_t_ref, new_i_ref, new_t_ref, grad_i_ref, grad_t_ref, sums_ref, dg_ref, db_ref,
                 tok_ref, cot_ref, y_i_ref, y_t_ref, acc_i_ref, acc_t_ref, hat_ref, inv_ref, nat_ref, trn_ref, v_ref, do_nat_ref, do_trn_ref, o_trn_ref, dq_ref, dk_ref, dv_ref):
    step_b, step_g = pl.program_id(0), pl.program_id(1)
    n_grp = pl.num_programs(1)
    n_img = hid_i_ref.shape[1]
    width = wq_ref.shape[2]
    head_dim = width // heads
    att_scale = head_dim ** -0.5
    n_tok = n_img + hid_t_ref.shape[1]
    k_rows = round_up(n_keys, 16)
    k_main = k_rows - 16

    @pl.when(step_g == 0)
    def _():
        tok_ref[...] = tok_i_ref[:, 0, 0].reshape(tok_ref.shape)
        cot_ref[...] = cot_i_ref[:, 0, 0].reshape(cot_ref.shape)
        prologue(tok_ref, cot_ref, mod_ref.at[0, 0], hid_i_ref.at[0], dy_i_ref.at[0], 16)
        prologue(tok_t_ref.at[0], cot_t_ref.at[0], mod_ref.at[0, 1], hid_t_ref.at[0], dy_t_ref.at[0], 16)
        hid_t_ref[0, n_keys - n_img:] = jnp.zeros((n_tok - n_keys, hid_t_ref.shape[2]), BF16)

    hid_i, hid_t = hid_i_ref[0], hid_t_ref[0]

    for idx, (w_ref, b_ref) in enumerate(((wq_ref, bq_ref), (wk_ref, bk_ref), (wv_ref, bv_ref))):
        raw_i = dot(hid_i, w_ref[0]) + b_ref[0:1, :]
        raw_t = dot(hid_t, w_ref[1]) + b_ref[1:2, :]
        if idx == 2:
            v_ref[:n_img] = raw_i.astype(BF16)
            v_ref[n_img:] = raw_t.astype(BF16)
            trn_ref[2, :, :n_img] = raw_i.T.astype(BF16)
            trn_ref[2, :, n_img:] = raw_t.T.astype(BF16)
        else:
            raw = jnp.concatenate([raw_i.T, raw_t.T], axis=1).reshape(heads, head_dim, n_tok)
            inv = lax.rsqrt(jnp.mean(raw * raw, axis=1, keepdims=True) + NORM_EPS)
            hat = (raw * inv).reshape(width, n_tok)
            normed = hat * gain_ref[idx]
            hat_ref[idx] = hat
            inv_ref[idx] = inv
            trn_ref[idx] = normed.astype(BF16)
            nat_ref[idx] = normed.T.astype(BF16)

    do_i = dot(dy_i_ref[0], wo_ref[0], NT)
    do_t = dot(dy_t_ref[0], wo_ref[1], NT)
    do_nat_ref[:n_img] = do_i.astype(BF16)
    do_nat_ref[n_img:] = do_t.astype(BF16)
    do_trn_ref[:, :n_img] = do_i.T.astype(BF16)
    do_trn_ref[:, n_img:] = do_t.T.astype(BF16)
    dk_ref[k_rows:] = jnp.zeros((n_tok - k_rows, width), F32)
    dv_ref[k_rows:] = jnp.zeros((n_tok - k_rows, width), F32)

    exp_scale = att_scale * math.log2(math.e)
    for head in range(heads):
        rows = slice(head * head_dim, (head + 1) * head_dim)
        q_trn, k_trn, v_trn = trn_ref[0, rows, :], trn_ref[1, rows, :k_rows], trn_ref[2, rows, :k_rows]
        q_nat, k_nat, v_nat = nat_ref[0, :, rows], nat_ref[1, :k_rows, rows], v_ref[:k_rows, rows]
        scores = dot(k_nat, q_trn)
        tail_row = k_main + lax.broadcasted_iota(jnp.int32, (16, n_tok), 0)
        tail = jnp.where(tail_row < n_keys, scores[k_main:], -jnp.inf)
        scores = jnp.concatenate([scores[:k_main], tail], axis=0)
        peak = jnp.max(scores, axis=0, keepdims=True)
        exps = jnp.exp2((scores - peak) * exp_scale)
        prob = exps * (1.0 / jnp.sum(exps, axis=0, keepdims=True))
        prob_lo = prob.astype(BF16)
        out_trn = dot(v_trn, prob_lo).astype(BF16)
        o_trn_ref[rows] = out_trn
        do_trn = do_trn_ref[rows]
        delta = jnp.sum(out_trn.astype(F32) * do_trn.astype(F32), axis=0, keepdims=True)
        d_prob = dot(v_nat, do_trn)
        d_score = (prob * (d_prob - delta)).astype(BF16)
        dv_ref[:k_rows, rows] = dot(prob_lo, do_nat_ref[:, rows])
        dk_ref[:k_rows, rows] = dot(d_score, q_nat) * att_scale
        dq_ref[rows] = dot(k_trn, d_score) * att_scale

    o_nat = o_trn_ref[...].astype(F32).T.astype(BF16)
    o_i_ref[0] = o_nat[:n_img]
    o_t_ref[0] = o_nat[n_img:]

    @pl.when(step_g == 0)
    def _():
        y_i_ref[...] = jnp.zeros_like(y_i_ref)
        y_t_ref[...] = jnp.zeros_like(y_t_ref)
        acc_i_ref[...] = jnp.zeros_like(acc_i_ref)
        acc_t_ref[...] = jnp.zeros_like(acc_t_ref)

    @pl.when((step_g == 0) & (step_b == 0))
    def _():
        dg_ref[...] = jnp.zeros_like(dg_ref)

    y_i_ref[...] += dot(o_nat[:n_img], wo_ref[0])
    y_t_ref[...] += dot(o_nat[n_img:], wo_ref[1])

    d_raw = []
    for idx in range(2):
        d_out = dq_ref[...] if idx == 0 else dk_ref[...].T
        d_out = d_out.astype(BF16).astype(F32)
        hat = hat_ref[idx]
        prod = d_out * hat
        dg_ref[idx] += sum(prod[:, lo:lo + 128] for lo in range(0, n_img, 128))
        dg_ref[2 + idx] += sum(prod[:, lo:lo + 128] for lo in range(n_img, n_tok, 128))
        d_hat = (d_out * gain_ref[idx]).reshape(heads, head_dim, n_tok)
        hat = hat.reshape(heads, head_dim, n_tok)
        mean_dh = jnp.mean(d_hat * hat, axis=1, keepdims=True)
        d_raw.append((inv_ref[idx] * (d_hat - hat * mean_dh)).reshape(width, n_tok).T)
    d_raw.append(dv_ref[...].astype(BF16).astype(F32))
    sums = []
    d_lo = []
    for idx in range(3):
        lo = d_raw[idx].astype(BF16)
        dp_i_ref[0, idx] = lo[:n_img]
        dp_t_ref[0, idx] = lo[n_img:]
        d_lo.append(lo)
        db_ref[0, idx:idx + 1, :] = jnp.sum(d_raw[idx][:n_img], axis=0, keepdims=True)
        db_ref[0, 3 + idx:4 + idx, :] = jnp.sum(d_raw[idx][n_img:], axis=0, keepdims=True)
    db_ref[0, 6:8, :] = jnp.zeros((2, width), F32)
    w_refs = (wq_ref, wk_ref, wv_ref)
    acc_i_ref[...] += sum(dot(d_lo[idx][:n_img], w_refs[idx][0], NT) for idx in range(3))
    acc_t_ref[...] += sum(dot(d_lo[idx][n_img:], w_refs[idx][1], NT) for idx in range(3))

    @pl.when(step_g == n_grp - 1)
    def _():
        epilogue(tok_ref, cot_ref, mod_ref.at[0, 0], bo_ref[0:1], y_i_ref, acc_i_ref, new_i_ref.at[0], grad_i_ref.at[0], sums_ref.at[0], 0, 16)
        epilogue(tok_t_ref.at[0], cot_t_ref.at[0], mod_ref.at[0, 1], bo_ref[1:2], y_t_ref, acc_t_ref, new_t_ref.at[0], grad_t_ref.at[0], sums_ref.at[0], 4, 16)


def fused_block(tokens, text, cot_t, mod, b_out, w_qkv, b_qkv, qk_gain, w_out, n_keys, heads):
    n_src, _, n_b, tok_dev, d_model = tokens.shape
    n_img, n_txt = n_src * tok_dev, text.shape[1]
    n_tok = n_img + n_txt
    head_dim = qk_gain.shape[-1]
    width = heads * head_dim
    n_grp = d_model // width
    gain_cols = jnp.tile(qk_gain, (1, 1, heads))
    gain_full = jnp.concatenate([jnp.broadcast_to(gain_cols[0][:, :, None], (2, width, n_img)), jnp.broadcast_to(gain_cols[1][:, :, None], (2, width, n_txt))], axis=2)

    def rows_spec(n_rows):
        return pl.BlockSpec((1, n_rows, d_model), lambda b, g: (b, 0, 0))

    def w_spec(idx):
        return pl.BlockSpec((2, d_model, width), lambda b, g: (0, 0, idx * n_grp + g))

    def b_spec(idx):
        return pl.BlockSpec((2, width), lambda b, g: (0, idx * n_grp + g))

    def img_spec(idx):
        return pl.BlockSpec((n_src, 1, 1, tok_dev, d_model), lambda b, g: (0, idx, b, 0, 0))

    in_specs = [img_spec(0), img_spec(1), rows_spec(n_txt), rows_spec(n_txt), pl.BlockSpec((1, 2, 3, d_model), lambda b, g: (b, 0, 0, 0)), pl.BlockSpec((2, d_model), lambda b, g: (0, 0)), w_spec(0), w_spec(1), w_spec(2), b_spec(0), b_spec(1), b_spec(2),
                pl.BlockSpec((2, width, n_tok), lambda b, g: (0, 0, 0)), pl.BlockSpec((2, width, d_model), lambda b, g: (0, g, 0))]
    out_specs = [rows_spec(n_img), rows_spec(n_txt), rows_spec(n_img), rows_spec(n_txt), pl.BlockSpec((1, n_img, width), lambda b, g: (b, 0, g)), pl.BlockSpec((1, n_txt, width), lambda b, g: (b, 0, g)),
                 pl.BlockSpec((1, 3, n_img, width), lambda b, g: (b, 0, 0, g)), pl.BlockSpec((1, 3, n_txt, width), lambda b, g: (b, 0, 0, g)),
                 rows_spec(n_img), rows_spec(n_txt), rows_spec(n_img), rows_spec(n_txt), pl.BlockSpec((1, 8, d_model), lambda b, g: (b, 0, 0)),
                 pl.BlockSpec((4, width, 128), lambda b, g: (0, 0, 0)), pl.BlockSpec((1, 8, width), lambda b, g: (b, 0, g))]
    shape = jax.ShapeDtypeStruct
    rows_shape = [shape((n_b, n_img, d_model), BF16), shape((n_b, n_txt, d_model), BF16)]
    out_shape = rows_shape * 3 + [
                 shape((n_b, 3, n_img, d_model), BF16), shape((n_b, 3, n_txt, d_model), BF16),
                 *(rows_shape * 2), shape((n_b, 8, d_model), F32),
                 shape((4, width, 128), F32), shape((n_b, 8, d_model), F32)]
    scratch = [pltpu.VMEM((n_img, d_model), BF16), pltpu.VMEM((n_img, d_model), BF16), pltpu.VMEM((n_img, d_model), F32), pltpu.VMEM((n_txt, d_model), F32), pltpu.VMEM((n_img, d_model), F32), pltpu.VMEM((n_txt, d_model), F32), pltpu.VMEM((2, width, n_tok), F32), pltpu.VMEM((2, heads, 1, n_tok), F32),
               pltpu.VMEM((2, n_tok, width), BF16), pltpu.VMEM((3, width, n_tok), BF16), pltpu.VMEM((n_tok, width), BF16),
               pltpu.VMEM((n_tok, width), BF16), pltpu.VMEM((width, n_tok), BF16), pltpu.VMEM((width, n_tok), BF16),
               pltpu.VMEM((width, n_tok), F32), pltpu.VMEM((n_tok, width), F32), pltpu.VMEM((n_tok, width), F32)]
    flops = n_b * n_tok * d_model * d_model * 16 + n_b * d_model * n_tok * n_tok * 12
    return pl.pallas_call(
        functools.partial(block_kernel, n_keys, heads),
        out_shape=out_shape, grid=(n_b, n_grp), in_specs=in_specs, out_specs=out_specs, scratch_shapes=scratch,
        compiler_params=pltpu.CompilerParams(dimension_semantics=("arbitrary", "arbitrary"), vmem_limit_bytes=67043328),
        cost_estimate=pl.CostEstimate(flops=flops, bytes_accessed=100 * 1024 * 1024, transcendentals=0),
        name="fused_block",
    )(tokens, tokens, text, cot_t, mod, b_out, w_qkv, w_qkv, w_qkv, b_qkv, b_qkv, b_qkv, gain_full, w_out)


def wgrad_kernel(core_ref, lo_i_ref, lp_i_ref, lo_t_ref, lp_t_ref, ro_i_ref, rp_i_ref, ro_t_ref, rp_t_ref, out_ref, trn_i_ref, trn_t_ref, rhs_i_ref, rhs_t_ref):
    branch, step = pl.program_id(0), pl.program_id(1)
    core = core_ref[0]

    def run(lo_ref, lp_ref, ro_ref, rp_ref, trn_ref, rhs_ref):
        n_b, n_rows, _ = lo_ref.shape

        @pl.when(step == 0)
        def _():
            for idx in range(n_b):
                trn_ref[:, pl.ds(pl.multiple_of((core * n_b + idx) * n_rows, n_rows), n_rows)] = lo_ref[idx].T
                trn_ref[:, pl.ds(pl.multiple_of(((1 - core) * n_b + idx) * n_rows, n_rows), n_rows)] = lp_ref[idx].T

        for idx in range(n_b):
            rhs_ref[pl.ds(pl.multiple_of((core * n_b + idx) * n_rows, n_rows), n_rows)] = ro_ref[idx, 0]
            rhs_ref[pl.ds(pl.multiple_of(((1 - core) * n_b + idx) * n_rows, n_rows), n_rows)] = rp_ref[idx, 0]
        out_ref[0] = dot(trn_ref[...], rhs_ref[...])

    @pl.when(branch == 0)
    def _():
        run(lo_i_ref, lp_i_ref, ro_i_ref, rp_i_ref, trn_i_ref, rhs_i_ref)

    @pl.when(branch == 1)
    def _():
        run(lo_t_ref, lp_t_ref, ro_t_ref, rp_t_ref, trn_t_ref, rhs_t_ref)


def wgrad(core, left_i, left_t, right_i, right_t, block, name):
    n_b, n_img, d_model = left_i[0].shape
    n_txt = left_t[0].shape[1]
    n_c = right_i[0].shape[1]
    per = right_i[0].shape[3] // block
    n_blk = n_c * per
    last = n_blk - 1

    def left_spec(n_rows):
        return pl.BlockSpec((n_b, n_rows, d_model), lambda s, j: (0, 0, 0), pipeline_mode=pl.Buffered(1))

    def img_map(s, j):
        pos = jnp.where(s == 0, j, last)
        return (0, pos // per, 0, pos % per)

    def txt_map(s, j):
        pos = jnp.where(s == 1, j, 0)
        return (0, pos // per, 0, pos % per)

    img_spec, txt_spec = pl.BlockSpec((n_b, 1, n_img, block), img_map), pl.BlockSpec((n_b, 1, n_txt, block), txt_map)
    in_specs = [pl.BlockSpec(memory_space=pltpu.SMEM), left_spec(n_img), left_spec(n_img), left_spec(n_txt), left_spec(n_txt), img_spec, img_spec, txt_spec, txt_spec]
    return pl.pallas_call(
        wgrad_kernel,
        out_shape=jax.ShapeDtypeStruct((2, d_model, n_blk * block), F32), grid=(2, n_blk), in_specs=in_specs,
        out_specs=pl.BlockSpec((1, d_model, block), lambda s, j: (s, 0, j)),
        scratch_shapes=[pltpu.VMEM((d_model, 2 * n_b * n_img), BF16), pltpu.VMEM((d_model, 2 * n_b * n_txt), BF16),
                        pltpu.VMEM((2 * n_b * n_img, block), BF16), pltpu.VMEM((2 * n_b * n_txt, block), BF16)],
        compiler_params=pltpu.CompilerParams(dimension_semantics=("arbitrary", "arbitrary"), vmem_limit_bytes=60 * 1024 * 1024),
        cost_estimate=pl.CostEstimate(flops=4 * n_b * (n_img + n_txt) * d_model * n_blk * block, bytes_accessed=8 * d_model * n_blk * block, transcendentals=0),
        name=name,
    )(core[None], *left_i, *left_t, *right_i, *right_t)


def ada_fwd_kernel(act_ref, w_ref, b_ref, out_ref):
    out_ref[0] = dot(act_ref[...], w_ref[0]) + b_ref[pl.ds(pl.program_id(0), 1), :]


def ada_fwd(cond_act, w_ada, b_ada, block):
    n_b, d_model = cond_act.shape
    wide = w_ada.shape[2]
    act = jnp.pad(cond_act, ((0, 16 - n_b), (0, 0)))
    return pl.pallas_call(
        ada_fwd_kernel,
        out_shape=jax.ShapeDtypeStruct((2, 16, wide), F32), grid=(2, wide // block),
        in_specs=[pl.BlockSpec((16, d_model), lambda s, j: (0, 0)), pl.BlockSpec((1, d_model, block), lambda s, j: (s, 0, j)), pl.BlockSpec((2, block), lambda s, j: (0, j))],
        out_specs=pl.BlockSpec((1, 16, block), lambda s, j: (s, 0, j)),
        compiler_params=pltpu.CompilerParams(dimension_semantics=("arbitrary", "arbitrary"), vmem_limit_bytes=40 * 1024 * 1024),
        cost_estimate=pl.CostEstimate(flops=64 * d_model * wide, bytes_accessed=4 * d_model * wide, transcendentals=0),
        name="ada_fwd",
    )(act, w_ada, b_ada)[:, :n_b]


def ada_bwd_kernel(act_ref, dmod_ref, w_ref, dw_ref, dact_ref):
    @pl.when((pl.program_id(0) == 0) & (pl.program_id(1) == 0))
    def _():
        dact_ref[...] = jnp.zeros_like(dact_ref)

    dmod = dmod_ref[0].astype(BF16)
    dw_ref[0] = dot(act_ref[...], dmod)
    dact_ref[...] += dot(dmod, w_ref[0], NT)


def ada_bwd(cond_act, d_mod, w_ada, block):
    n_b, d_model = cond_act.shape
    wide = w_ada.shape[2]
    act_trn = jnp.pad(cond_act, ((0, 16 - n_b), (0, 0))).T
    d_mod = jnp.pad(d_mod, ((0, 0), (0, 16 - n_b), (0, 0)))
    dw_ada, d_act = pl.pallas_call(
        ada_bwd_kernel,
        out_shape=[jax.ShapeDtypeStruct(w_ada.shape, F32), jax.ShapeDtypeStruct((16, d_model), F32)], grid=(2, wide // block),
        in_specs=[pl.BlockSpec((d_model, 16), lambda s, j: (0, 0)), pl.BlockSpec((1, 16, block), lambda s, j: (s, 0, j)), pl.BlockSpec((1, d_model, block), lambda s, j: (s, 0, j))],
        out_specs=[pl.BlockSpec((1, d_model, block), lambda s, j: (s, 0, j)), pl.BlockSpec((16, d_model), lambda s, j: (0, 0))],
        compiler_params=pltpu.CompilerParams(dimension_semantics=("arbitrary", "arbitrary"), vmem_limit_bytes=40 * 1024 * 1024),
        cost_estimate=pl.CostEstimate(flops=8 * d_model * wide * 16, bytes_accessed=12 * d_model * wide, transcendentals=0),
        name="ada_bwd",
    )(act_trn, d_mod, w_ada)
    return dw_ada, d_act[:n_b]


def solution(mesh):
    sp_size = mesh.shape['sp']
    pair = 2
    n_chips = sp_size // pair
    pairs = [(idx, idx + 1 - 2 * (idx % pair)) for idx in range(sp_size)]

    def swap(arr):
        return lax.ppermute(arr, 'sp', pairs)

    def both(arr):
        return arr, swap(arr)

    def device_fn(image_in, text_in, cond_vec, w_ada, b_ada, w_qkv, b_qkv, qk_gain, w_out, b_out, image_cot, text_cot):
        n_batch, tok_dev, d_model = image_in.shape
        ctx_len = text_in.shape[1]
        n_img = tok_dev * sp_size
        n_own = n_batch // pair
        n_txt = round_up(n_img + ctx_len, 128) - n_img
        me = lax.axis_index('sp')
        core, chip = lax.rem(me, pair), lax.div(me, pair)
        own_lo = core * n_own

        tokens = jnp.stack([image_in, image_cot]).reshape(2, pair, n_own, tok_dev, d_model).swapaxes(0, 1)
        tokens = jnp.concatenate([tokens] * n_chips, axis=0)
        tokens = lax.all_to_all(tokens, 'sp', 0, 0)

        def own(arr, axis=0):
            return lax.dynamic_slice_in_dim(arr, own_lo, n_own, axis)

        def ordered(mine, other, axis=0):
            return jnp.where(core == 0, jnp.concatenate([mine, other], axis), jnp.concatenate([other, mine], axis))

        cond_act = jax.nn.silu(cond_vec.astype(F32)).astype(BF16)
        cond_mod = ada_fwd(cond_act, w_ada, b_ada, 1536)
        own_mod = own(cond_mod, 1).reshape(2, n_own, 3, d_model).swapaxes(0, 1)
        pad_rows = ((0, 0), (0, n_txt - ctx_len), (0, 0))
        text_own, cot_own = jnp.pad(own(text_in), pad_rows), jnp.pad(own(text_cot), pad_rows)

        hid_i, hid_t, dy_i, dy_t, o_i, o_t, dp_i, dp_t, new_i, new_t, grad_i, grad_t, sums, dg, db = fused_block(
            tokens, text_own, cot_own, own_mod, b_out, w_qkv, b_qkv, qk_gain, w_out, n_img + ctx_len, 4)

        sums = sums.reshape(n_own, 2, 4, d_model)
        d_mod = sums[:, :, :3].swapaxes(0, 1).reshape(2, n_own, 3 * d_model)
        rest = jnp.concatenate([jnp.sum(sums[:, :, 3], 0).reshape(-1), jnp.sum(db, 0)[:6].reshape(-1), jnp.sum(jnp.sum(dg, -1).reshape(2, 2, -1, qk_gain.shape[-1]), 2).reshape(-1)])
        small = jnp.concatenate([d_mod.reshape(-1), rest])
        small_other = swap(small)
        d_mod_all = ordered(d_mod, small_other[:d_mod.size].reshape(d_mod.shape), 1)
        rest = rest + small_other[d_mod.size:]
        cut = (2 * d_model, 8 * d_model)
        db_out, db_qkv, d_gain = rest[:cut[0]].reshape(2, d_model), rest[cut[0]:cut[1]].reshape(2, 3 * d_model), rest[cut[1]:].reshape(qk_gain.shape)

        o_i, o_t, dy_i, dy_t = both(o_i), both(o_t), both(dy_i[:, None]), both(dy_t[:, None])
        hid_i, hid_t, dp_i, dp_t = both(hid_i), both(hid_t), both(dp_i), both(dp_t)
        dw_ada, d_act = ada_bwd(cond_act, d_mod_all, w_ada, 512)
        dw_out = wgrad(core, o_i, o_t, dy_i, dy_t, 512, "wgrad_out")
        dw_qkv = wgrad(core, hid_i, hid_t, dp_i, dp_t, 512, "wgrad_qkv")
        db_ada = jnp.sum(d_mod_all, axis=1)
        _, pull_act = jax.vjp(jax.nn.silu, cond_vec.astype(F32))
        grad_cond = pull_act(d_act.astype(BF16).astype(F32))[0]

        img_pair = jnp.stack([new_i, grad_i], axis=1)
        chip_lo = chip * pair * tok_dev
        img_mine = lax.dynamic_slice_in_dim(img_pair, chip_lo + core * tok_dev, tok_dev, 2)
        img_send = lax.dynamic_slice_in_dim(img_pair, chip_lo + (1 - core) * tok_dev, tok_dev, 2)
        img_pair = ordered(img_mine, swap(img_send))
        text_new, grad_text = ordered(*both(new_t[:, :ctx_len])), ordered(*both(grad_t[:, :ctx_len]))
        return (img_pair[:, 0], text_new, img_pair[:, 1], grad_text, grad_cond, dw_ada, db_ada, dw_qkv, db_qkv, d_gain, dw_out, db_out)

    data_spec = P('dp', 'sp', None)
    batch_spec = P('dp')
    rep_spec = P()
    in_specs = (data_spec, batch_spec, batch_spec, rep_spec, rep_spec, rep_spec, rep_spec, rep_spec, rep_spec, rep_spec, data_spec, batch_spec)
    out_specs = (data_spec, batch_spec, data_spec, batch_spec, batch_spec, batch_spec, batch_spec, batch_spec, batch_spec, batch_spec, batch_spec, batch_spec)
    return jax.shard_map(device_fn, mesh=mesh, in_specs=in_specs, out_specs=out_specs, check_vma=False)
```

```python
import functools
import math
import jax
import jax.numpy as jnp
from jax import lax
from jax.experimental import pallas as pl
from jax.experimental.pallas import tpu as pltpu
from jax.sharding import PartitionSpec as P

NORM_EPS = 1e-6
F32 = jnp.float32
BF16 = jnp.bfloat16
NN = (((1,), (0,)), ((), ()))
NT = (((1,), (1,)), ((), ()))
TN = (((0,), (0,)), ((), ()))


def dot(lhs, rhs, dims=NN):
    return lax.dot_general(lhs, rhs, dims, preferred_element_type=F32)


def round_up(num, mult):
    return -(-num // mult) * mult


def stats(tokens):
    avg_val = jnp.mean(tokens, axis=-1, keepdims=True)
    centred = tokens - avg_val
    var_val = jnp.mean(centred * centred, axis=-1, keepdims=True)
    inv_std = lax.rsqrt(var_val + NORM_EPS)
    return centred * inv_std, inv_std


def prologue(tok_ref, cot_ref, mod_ref, hid_ref, hid_trn_ref, dy_ref, base, n_valid, chunk):
    @pl.loop(0, tok_ref.shape[0] // chunk)
    def _(step):
        rows = pl.ds(pl.multiple_of(step * chunk, chunk), chunk)
        dst = pl.ds(pl.multiple_of(base + step * chunk, chunk), chunk)
        normed, _ = stats(tok_ref[rows].astype(F32))
        hid = normed * (1.0 + mod_ref[1:2]) + mod_ref[0:1]
        if n_valid < tok_ref.shape[0]:
            row = step * chunk + lax.broadcasted_iota(jnp.int32, hid.shape, 0)
            hid = jnp.where(row < n_valid, hid, 0.0)
        hid = hid.astype(BF16)
        hid_ref[dst] = hid
        hid_trn_ref[:, dst] = hid.T
        dy_ref[dst] = (cot_ref[rows].astype(F32) * mod_ref[2:3]).astype(BF16)


def epilogue(tok_ref, cot_ref, mod_ref, bias, y_ref, acc_ref, new_ref, grad_ref, sums_ref, base, chunk):
    sums_ref[base:base + 4] = jnp.zeros((4, sums_ref.shape[1]), F32)

    @pl.loop(0, tok_ref.shape[0] // chunk)
    def _(step):
        rows = pl.ds(pl.multiple_of(step * chunk, chunk), chunk)
        tokens, cot = tok_ref[rows].astype(F32), cot_ref[rows].astype(F32)
        gate = mod_ref[2:3]
        y_out = y_ref[rows] + bias
        new_ref[rows] = (tokens + gate * y_out).astype(BF16)
        normed, inv_std = stats(tokens)
        d_hid = acc_ref[rows].astype(BF16).astype(F32)
        d_normed = d_hid * (1.0 + mod_ref[1:2])
        mean_d = jnp.mean(d_normed, axis=-1, keepdims=True)
        mean_dn = jnp.mean(d_normed * normed, axis=-1, keepdims=True)
        grad_ref[rows] = (cot + inv_std * (d_normed - mean_d - normed * mean_dn)).astype(BF16)
        sums_ref[base:base + 1] += jnp.sum(d_hid, axis=0, keepdims=True)
        sums_ref[base + 1:base + 2] += jnp.sum(d_hid * normed, axis=0, keepdims=True)
        sums_ref[base + 2:base + 3] += jnp.sum(cot * y_out, axis=0, keepdims=True)
        sums_ref[base + 3:base + 4] += jnp.sum(cot * gate, axis=0, keepdims=True)


def block_kernel(n_keys, heads, tok_i_ref, cot_i_ref, tok_t_ref, cot_t_ref, mod_ref, bo_ref, wq_ref, wk_ref, wv_ref, bq_ref, bk_ref, bv_ref, gain_ref, wo_ref,
                 hid_trn_ref, dy_ref, o_trn_ref, dp_ref, new_i_ref, new_t_ref, grad_i_ref, grad_t_ref, sums_ref, dg_ref, db_ref,
                 hid_ref, tok_ref, cot_ref, y_i_ref, y_t_ref, acc_i_ref, acc_t_ref, hat_ref, inv_ref, nat_ref, trn_ref, v_ref, do_nat_ref, do_trn_ref, dq_ref, dk_ref, dv_ref):
    step_b, step_g = pl.program_id(0), pl.program_id(1)
    n_grp = pl.num_programs(1)
    n_img = tok_ref.shape[0]
    width = wq_ref.shape[2]
    head_dim = width // heads
    att_scale = head_dim ** -0.5
    n_tok = n_img + tok_t_ref.shape[1]
    k_rows = round_up(n_keys, 16)
    k_main = k_rows - 16

    @pl.when(step_g == 0)
    def _():
        tok_ref[...] = tok_i_ref[:, 0, 0].reshape(tok_ref.shape)
        cot_ref[...] = cot_i_ref[:, 0, 0].reshape(cot_ref.shape)
        prologue(tok_ref, cot_ref, mod_ref.at[0, 0], hid_ref, hid_trn_ref.at[0], dy_ref.at[0], 0, n_img, 128)
        prologue(tok_t_ref.at[0], cot_t_ref.at[0], mod_ref.at[0, 1], hid_ref, hid_trn_ref.at[0], dy_ref.at[0], n_img, n_keys - n_img, 128)

    hid_i, hid_t = hid_ref[:n_img], hid_ref[n_img:]
    for idx, (w_ref, b_ref) in enumerate(((wq_ref, bq_ref), (wk_ref, bk_ref), (wv_ref, bv_ref))):
        raw_i = dot(hid_i, w_ref[0]) + b_ref[0:1, :]
        raw_t = dot(hid_t, w_ref[1]) + b_ref[1:2, :]
        if idx == 2:
            v_ref[:n_img] = raw_i.astype(BF16)
            v_ref[n_img:] = raw_t.astype(BF16)
            trn_ref[2, :, :n_img] = raw_i.T.astype(BF16)
            trn_ref[2, :, n_img:] = raw_t.T.astype(BF16)
        else:
            raw = jnp.concatenate([raw_i.T, raw_t.T], axis=1).reshape(heads, head_dim, n_tok)
            inv = lax.rsqrt(jnp.mean(raw * raw, axis=1, keepdims=True) + NORM_EPS)
            hat = (raw * inv).reshape(width, n_tok)
            normed = hat * gain_ref[idx]
            hat_ref[idx] = hat
            inv_ref[idx] = inv
            trn_ref[idx] = normed.astype(BF16)
            nat_ref[idx] = normed.T.astype(BF16)

    do_i = dot(dy_ref[0, :n_img], wo_ref[0], NT)
    do_t = dot(dy_ref[0, n_img:], wo_ref[1], NT)
    do_nat_ref[:n_img] = do_i.astype(BF16)
    do_nat_ref[n_img:] = do_t.astype(BF16)
    do_trn_ref[:, :n_img] = do_i.T.astype(BF16)
    do_trn_ref[:, n_img:] = do_t.T.astype(BF16)
    dk_ref[k_rows:] = jnp.zeros((n_tok - k_rows, width), F32)
    dv_ref[k_rows:] = jnp.zeros((n_tok - k_rows, width), F32)

    exp_scale = att_scale * math.log2(math.e)
    for head in range(heads):
        rows = slice(head * head_dim, (head + 1) * head_dim)
        q_trn, k_trn, v_trn = trn_ref[0, rows, :], trn_ref[1, rows, :k_rows], trn_ref[2, rows, :k_rows]
        q_nat, k_nat, v_nat = nat_ref[0, :, rows], nat_ref[1, :k_rows, rows], v_ref[:k_rows, rows]
        scores = dot(k_nat, q_trn)
        tail_row = k_main + lax.broadcasted_iota(jnp.int32, (16, n_tok), 0)
        tail = jnp.where(tail_row < n_keys, scores[k_main:], -jnp.inf)
        scores = jnp.concatenate([scores[:k_main], tail], axis=0)
        peak = jnp.max(scores, axis=0, keepdims=True)
        exps = jnp.exp2((scores - peak) * exp_scale)
        prob = exps * (1.0 / jnp.sum(exps, axis=0, keepdims=True))
        prob_lo = prob.astype(BF16)
        out_trn = dot(v_trn, prob_lo).astype(BF16)
        o_trn_ref[0, rows] = out_trn
        do_trn = do_trn_ref[rows]
        delta = jnp.sum(out_trn.astype(F32) * do_trn.astype(F32), axis=0, keepdims=True)
        d_prob = dot(v_nat, do_trn)
        d_score = (prob * (d_prob - delta)).astype(BF16)
        dv_ref[:k_rows, rows] = dot(prob_lo, do_nat_ref[:, rows])
        dk_ref[:k_rows, rows] = dot(d_score, q_nat) * att_scale
        dq_ref[rows] = dot(k_trn, d_score) * att_scale

    o_nat = o_trn_ref[0].T

    @pl.when(step_g == 0)
    def _():
        y_i_ref[...] = jnp.zeros_like(y_i_ref)
        y_t_ref[...] = jnp.zeros_like(y_t_ref)
        acc_i_ref[...] = jnp.zeros_like(acc_i_ref)
        acc_t_ref[...] = jnp.zeros_like(acc_t_ref)

    @pl.when((step_g == 0) & (step_b == 0))
    def _():
        dg_ref[...] = jnp.zeros_like(dg_ref)

    y_i_ref[...] += dot(o_nat[:n_img], wo_ref[0])
    y_t_ref[...] += dot(o_nat[n_img:], wo_ref[1])

    d_raw = []
    for idx in range(2):
        d_out = dq_ref[...] if idx == 0 else dk_ref[...].T
        d_out = d_out.astype(BF16).astype(F32)
        hat = hat_ref[idx]
        prod = d_out * hat
        dg_ref[idx] += sum(prod[:, lo:lo + 128] for lo in range(0, n_img, 128))
        dg_ref[2 + idx] += sum(prod[:, lo:lo + 128] for lo in range(n_img, n_tok, 128))
        d_hat = (d_out * gain_ref[idx]).reshape(heads, head_dim, n_tok)
        hat = hat.reshape(heads, head_dim, n_tok)
        mean_dh = jnp.mean(d_hat * hat, axis=1, keepdims=True)
        d_raw.append((inv_ref[idx] * (d_hat - hat * mean_dh)).reshape(width, n_tok).T)
    d_raw.append(dv_ref[...].astype(BF16).astype(F32))
    sums = []
    d_lo = []
    for idx in range(3):
        lo = d_raw[idx].astype(BF16)
        dp_ref[0, idx] = lo
        d_lo.append(lo)
        db_ref[0, idx:idx + 1, :] = jnp.sum(d_raw[idx][:n_img], axis=0, keepdims=True)
        db_ref[0, 3 + idx:4 + idx, :] = jnp.sum(d_raw[idx][n_img:], axis=0, keepdims=True)
    db_ref[0, 6:8, :] = jnp.zeros((2, width), F32)
    w_refs = (wq_ref, wk_ref, wv_ref)
    acc_i_ref[...] += sum(dot(d_lo[idx][:n_img], w_refs[idx][0], NT) for idx in range(3))
    acc_t_ref[...] += sum(dot(d_lo[idx][n_img:], w_refs[idx][1], NT) for idx in range(3))

    @pl.when(step_g == n_grp - 1)
    def _():
        epilogue(tok_ref, cot_ref, mod_ref.at[0, 0], bo_ref[0:1], y_i_ref, acc_i_ref, new_i_ref.at[0], grad_i_ref.at[0], sums_ref.at[0], 0, 64)
        epilogue(tok_t_ref.at[0], cot_t_ref.at[0], mod_ref.at[0, 1], bo_ref[1:2], y_t_ref, acc_t_ref, new_t_ref.at[0], grad_t_ref.at[0], sums_ref.at[0], 4, 64)


def fused_block(tokens, text, cot_t, mod, b_out, w_qkv, b_qkv, qk_gain, w_out, n_keys, heads):
    n_src, _, n_b, tok_dev, d_model = tokens.shape
    n_img, n_txt = n_src * tok_dev, text.shape[1]
    n_tok = n_img + n_txt
    head_dim = qk_gain.shape[-1]
    width = heads * head_dim
    n_grp = d_model // width
    gain_cols = jnp.tile(qk_gain, (1, 1, heads))
    gain_full = jnp.concatenate([jnp.broadcast_to(gain_cols[0][:, :, None], (2, width, n_img)), jnp.broadcast_to(gain_cols[1][:, :, None], (2, width, n_txt))], axis=2)

    def rows_spec(n_rows, **mode):
        return pl.BlockSpec((1, n_rows, d_model), lambda b, g: (b, 0, 0), **mode)

    def w_spec(idx):
        return pl.BlockSpec((2, d_model, width), lambda b, g: (0, 0, idx * n_grp + g))

    def b_spec(idx):
        return pl.BlockSpec((2, width), lambda b, g: (0, idx * n_grp + g))

    def img_spec(idx):
        return pl.BlockSpec((n_src, 1, 1, tok_dev, d_model), lambda b, g: (0, idx, b, 0, 0), pipeline_mode=pl.Buffered(1))

    once = pl.Buffered(1)
    in_specs = [img_spec(0), img_spec(1), rows_spec(n_txt, pipeline_mode=once), rows_spec(n_txt, pipeline_mode=once), pl.BlockSpec((1, 2, 3, d_model), lambda b, g: (b, 0, 0, 0)), pl.BlockSpec((2, d_model), lambda b, g: (0, 0)), w_spec(0), w_spec(1), w_spec(2), b_spec(0), b_spec(1), b_spec(2),
                pl.BlockSpec((2, width, n_tok), lambda b, g: (0, 0, 0)), pl.BlockSpec((2, width, d_model), lambda b, g: (0, g, 0))]
    out_specs = [pl.BlockSpec((1, d_model, n_tok), lambda b, g: (b, 0, 0)), rows_spec(n_tok), pl.BlockSpec((1, width, n_tok), lambda b, g: (b, g, 0)), pl.BlockSpec((1, 3, n_tok, width), lambda b, g: (b, 0, 0, g)),
                 rows_spec(n_img), rows_spec(n_txt), rows_spec(n_img), rows_spec(n_txt), pl.BlockSpec((1, 8, d_model), lambda b, g: (b, 0, 0)),
                 pl.BlockSpec((4, width, 128), lambda b, g: (0, 0, 0)), pl.BlockSpec((1, 8, width), lambda b, g: (b, 0, g))]
    shape = jax.ShapeDtypeStruct
    rows_shape = [shape((n_b, n_img, d_model), BF16), shape((n_b, n_txt, d_model), BF16)]
    out_shape = [shape((n_b, d_model, n_tok), BF16), shape((n_b, n_tok, d_model), BF16), shape((n_b, d_model, n_tok), BF16), shape((n_b, 3, n_tok, d_model), BF16),
                 *(rows_shape * 2), shape((n_b, 8, d_model), F32), shape((4, width, 128), F32), shape((n_b, 8, d_model), F32)]
    scratch = [pltpu.VMEM((n_tok, d_model), BF16), pltpu.VMEM((n_img, d_model), BF16), pltpu.VMEM((n_img, d_model), BF16),
               pltpu.VMEM((n_img, d_model), F32), pltpu.VMEM((n_txt, d_model), F32), pltpu.VMEM((n_img, d_model), F32), pltpu.VMEM((n_txt, d_model), F32),
               pltpu.VMEM((2, width, n_tok), F32), pltpu.VMEM((2, heads, 1, n_tok), F32),
               pltpu.VMEM((2, n_tok, width), BF16), pltpu.VMEM((3, width, n_tok), BF16), pltpu.VMEM((n_tok, width), BF16),
               pltpu.VMEM((n_tok, width), BF16), pltpu.VMEM((width, n_tok), BF16),
               pltpu.VMEM((width, n_tok), F32), pltpu.VMEM((n_tok, width), F32), pltpu.VMEM((n_tok, width), F32)]
    flops = n_b * n_tok * d_model * d_model * 16 + n_b * d_model * n_tok * n_tok * 12
    return pl.pallas_call(
        functools.partial(block_kernel, n_keys, heads),
        out_shape=out_shape, grid=(n_b, n_grp), in_specs=in_specs, out_specs=out_specs, scratch_shapes=scratch,
        compiler_params=pltpu.CompilerParams(dimension_semantics=("arbitrary", "arbitrary"), vmem_limit_bytes=67043328),
        cost_estimate=pl.CostEstimate(flops=flops, bytes_accessed=100 * 1024 * 1024, transcendentals=0),
        name="fused_block",
    )(tokens, tokens, text, cot_t, mod, b_out, w_qkv, w_qkv, w_qkv, b_qkv, b_qkv, b_qkv, gain_full, w_out)


def wgrad_kernel(n_img, n_b, with_ada, core_ref, *refs):
    lefts, rights, refs = refs[:2 * n_b], refs[2 * n_b:4 * n_b], refs[4 * n_b:]
    if with_ada:
        act_ref, dmod_ref, dmod_trn_ref, w_ref, out_ref, dw_ref, dact_ref, trn_i_ref, trn_t_ref, rhs_i_ref, rhs_t_ref = refs
    else:
        out_ref, trn_i_ref, trn_t_ref, rhs_i_ref, rhs_t_ref = refs
    d_model, n_tok = lefts[0].shape[1:]
    n_txt = n_tok - n_img
    core = core_ref[0]

    def place(idx, n_rows):
        pos = core * n_b + idx if idx < n_b else (1 - core) * n_b + idx - n_b
        return pl.ds(pl.multiple_of(pos * n_rows, n_rows), n_rows)

    @pl.when(pl.program_id(0) == 0)
    def _():
        for idx in range(2 * n_b):
            trn_i_ref[:, place(idx, n_img)] = lefts[idx][0, :, :n_img]
            trn_t_ref[:, place(idx, n_txt)] = lefts[idx][0, :, n_img:]
        if with_ada:
            dact_ref[...] = jnp.zeros_like(dact_ref)

    for idx in range(2 * n_b):
        rhs_i_ref[place(idx, n_img)] = rights[idx][0, 0, :n_img]
        rhs_t_ref[place(idx, n_txt)] = rights[idx][0, 0, n_img:]

    chunk = 512

    @pl.loop(0, d_model // chunk)
    def _(step):
        rows = pl.ds(pl.multiple_of(step * chunk, chunk), chunk)
        out_ref[0, rows] = dot(trn_i_ref[rows], rhs_i_ref[...])
        out_ref[1, rows] = dot(trn_t_ref[rows], rhs_t_ref[...])
        if with_ada:
            for branch in range(2):
                dw_ref[branch, rows] = dot(act_ref[rows], dmod_ref[branch].astype(BF16))
                dact_ref[rows] += dot(w_ref[branch, rows], dmod_trn_ref[branch].astype(BF16))


def wgrad(core, lefts, rights, n_img, block, name, ada=None):
    n_b = len(lefts) // 2
    _, d_model, n_tok = lefts[0].shape
    n_c, wide = rights[0].shape[1], rights[0].shape[3]
    per = wide // block
    cols = n_c * wide
    left_spec = pl.BlockSpec((1, d_model, n_tok), lambda j: (0, 0, 0), pipeline_mode=pl.Buffered(1))
    right_spec = pl.BlockSpec((1, 1, n_tok, block), lambda j: (0, j // per, 0, j % per))
    mat_spec = pl.BlockSpec((2, d_model, block), lambda j: (0, 0, j))
    in_specs = [pl.BlockSpec(memory_space=pltpu.SMEM)] + [left_spec] * (2 * n_b) + [right_spec] * (2 * n_b)
    out_shape, out_specs, extra = [jax.ShapeDtypeStruct((2, d_model, cols), F32)], [mat_spec], []
    if ada is not None:
        cond_act, d_mod, w_ada = ada
        n_batch = cond_act.shape[0]
        d_mod = jnp.pad(d_mod, ((0, 0), (0, 16 - n_batch), (0, 0)))
        extra = [jnp.pad(cond_act, ((0, 16 - n_batch), (0, 0))).T, d_mod, d_mod.swapaxes(1, 2), w_ada]
        in_specs += [pl.BlockSpec((d_model, 16), lambda j: (0, 0)), pl.BlockSpec((2, 16, block), lambda j: (0, 0, j)), pl.BlockSpec((2, block, 16), lambda j: (0, j, 0)), mat_spec]
        out_shape += [jax.ShapeDtypeStruct((2, d_model, cols), F32), jax.ShapeDtypeStruct((d_model, 16), F32)]
        out_specs += [mat_spec, pl.BlockSpec((d_model, 16), lambda j: (0, 0))]
    return pl.pallas_call(
        functools.partial(wgrad_kernel, n_img, n_b, ada is not None),
        out_shape=out_shape, grid=(n_c * per,), in_specs=in_specs, out_specs=out_specs,
        scratch_shapes=[pltpu.VMEM((d_model, 2 * n_b * n_img), BF16), pltpu.VMEM((d_model, 2 * n_b * (n_tok - n_img)), BF16),
                        pltpu.VMEM((2 * n_b * n_img, block), BF16), pltpu.VMEM((2 * n_b * (n_tok - n_img), block), BF16)],
        compiler_params=pltpu.CompilerParams(dimension_semantics=("arbitrary",), vmem_limit_bytes=60 * 1024 * 1024),
        cost_estimate=pl.CostEstimate(flops=4 * n_b * n_tok * d_model * cols, bytes_accessed=(8 if ada is None else 24) * d_model * cols, transcendentals=0),
        name=name,
    )(core[None], *lefts, *rights, *extra)


def ada_fwd_kernel(act_ref, w_ref, b_ref, out_ref):
    out_ref[0] = dot(act_ref[...], w_ref[0]) + b_ref[pl.ds(pl.program_id(0), 1), :]


def ada_fwd(cond_act, w_ada, b_ada, block):
    n_b, d_model = cond_act.shape
    wide = w_ada.shape[2]
    act = jnp.pad(cond_act, ((0, 16 - n_b), (0, 0)))
    return pl.pallas_call(
        ada_fwd_kernel,
        out_shape=jax.ShapeDtypeStruct((2, 16, wide), F32), grid=(2, wide // block),
        in_specs=[pl.BlockSpec((16, d_model), lambda s, j: (0, 0)), pl.BlockSpec((1, d_model, block), lambda s, j: (s, 0, j)), pl.BlockSpec((2, block), lambda s, j: (0, j))],
        out_specs=pl.BlockSpec((1, 16, block), lambda s, j: (s, 0, j)),
        compiler_params=pltpu.CompilerParams(dimension_semantics=("arbitrary", "arbitrary"), vmem_limit_bytes=40 * 1024 * 1024),
        cost_estimate=pl.CostEstimate(flops=64 * d_model * wide, bytes_accessed=4 * d_model * wide, transcendentals=0),
        name="ada_fwd",
    )(act, w_ada, b_ada)[:, :n_b]


def solution(mesh):
    sp_size = mesh.shape['sp']
    pair = 2
    n_chips = sp_size // pair
    pairs = [(idx, idx + 1 - 2 * (idx % pair)) for idx in range(sp_size)]

    def swap(arr):
        return lax.ppermute(arr, 'sp', pairs)

    def both(arr):
        return arr, swap(arr)

    def device_fn(image_in, text_in, cond_vec, w_ada, b_ada, w_qkv, b_qkv, qk_gain, w_out, b_out, image_cot, text_cot):
        n_batch, tok_dev, d_model = image_in.shape
        ctx_len = text_in.shape[1]
        n_img = tok_dev * sp_size
        n_own = n_batch // pair
        n_txt = round_up(n_img + ctx_len, 128) - n_img
        me = lax.axis_index('sp')
        core, chip = lax.rem(me, pair), lax.div(me, pair)
        own_lo = core * n_own

        img_pair = jnp.stack([image_in, image_cot]).reshape(2, pair, n_own, 1, tok_dev, d_model)
        tokens = [lax.all_to_all(jnp.concatenate([img_pair[:, :, idx].swapaxes(0, 1)] * n_chips, axis=0), 'sp', 0, 0) for idx in range(n_own)]

        def own(arr, axis=0):
            return lax.dynamic_slice_in_dim(arr, own_lo, n_own, axis)

        def ordered(mine, other, axis=0):
            return jnp.where(core == 0, jnp.concatenate([mine, other], axis), jnp.concatenate([other, mine], axis))

        cond_act = jax.nn.silu(cond_vec.astype(F32)).astype(BF16)
        cond_mod = ada_fwd(cond_act, w_ada, b_ada, 1536)
        own_mod = own(cond_mod, 1).reshape(2, n_own, 3, d_model).swapaxes(0, 1)
        pad_rows = ((0, 0), (0, n_txt - ctx_len), (0, 0))
        text_own, cot_own = jnp.pad(own(text_in), pad_rows), jnp.pad(own(text_cot), pad_rows)

        outs = []
        for idx in range(n_own):
            one = slice(idx, idx + 1)
            outs.append(fused_block(tokens[idx], text_own[one], cot_own[one], own_mod[one], b_out, w_qkv, b_qkv, qk_gain, w_out, n_img + ctx_len, 4))
        sums, db = (jnp.concatenate([out[pos] for out in outs]) for pos in (8, 10))
        new_i, new_t, grad_i, grad_t = (jnp.concatenate([out[pos] for out in outs]) for pos in (4, 5, 6, 7))
        dg = sum(out[9] for out in outs)
        factors = [[out[pos] for out in outs] for pos in range(4)]
        factors[1] = [arr[:, None] for arr in factors[1]]
        hid_trn, dy, o_trn, dp = [arrs + [swap(arr) for arr in arrs] for arrs in factors]

        sums = sums.reshape(n_own, 2, 4, d_model)
        d_mod = sums[:, :, :3].swapaxes(0, 1).reshape(2, n_own, 3 * d_model)
        rest = jnp.concatenate([jnp.sum(sums[:, :, 3], 0).reshape(-1), jnp.sum(db, 0)[:6].reshape(-1), jnp.sum(jnp.sum(dg, -1).reshape(2, 2, -1, qk_gain.shape[-1]), 2).reshape(-1)])
        small = jnp.concatenate([d_mod.reshape(-1), rest])
        small_other = swap(small)
        d_mod_all = ordered(d_mod, small_other[:d_mod.size].reshape(d_mod.shape), 1)
        rest = rest + small_other[d_mod.size:]
        cut = (2 * d_model, 8 * d_model)
        db_out, db_qkv, d_gain = rest[:cut[0]].reshape(2, d_model), rest[cut[0]:cut[1]].reshape(2, 3 * d_model), rest[cut[1]:].reshape(qk_gain.shape)

        dw_out, = wgrad(core, o_trn, dy, n_img, 256, "wgrad_out")
        dw_qkv, dw_ada, d_act = wgrad(core, hid_trn, dp, n_img, 256, "wgrad_qkv", (cond_act, d_mod_all, w_ada))
        d_act = d_act.T[:n_batch]
        db_ada = jnp.sum(d_mod_all, axis=1)
        _, pull_act = jax.vjp(jax.nn.silu, cond_vec.astype(F32))
        grad_cond = pull_act(d_act.astype(BF16).astype(F32))[0]

        img_pair = jnp.stack([new_i, grad_i], axis=1)
        chip_lo = chip * pair * tok_dev
        img_mine = lax.dynamic_slice_in_dim(img_pair, chip_lo + core * tok_dev, tok_dev, 2)
        img_send = lax.dynamic_slice_in_dim(img_pair, chip_lo + (1 - core) * tok_dev, tok_dev, 2)
        img_pair = ordered(img_mine, swap(img_send))
        text_new, grad_text = ordered(*both(new_t[:, :ctx_len])), ordered(*both(grad_t[:, :ctx_len]))
        return (img_pair[:, 0], text_new, img_pair[:, 1], grad_text, grad_cond, dw_ada, db_ada, dw_qkv, db_qkv, d_gain, dw_out, db_out)

    data_spec = P('dp', 'sp', None)
    batch_spec = P('dp')
    rep_spec = P()
    in_specs = (data_spec, batch_spec, batch_spec, rep_spec, rep_spec, rep_spec, rep_spec, rep_spec, rep_spec, rep_spec, data_spec, batch_spec)
    out_specs = (data_spec, batch_spec, data_spec, batch_spec, batch_spec, batch_spec, batch_spec, batch_spec, batch_spec, batch_spec, batch_spec, batch_spec)
    return jax.shard_map(device_fn, mesh=mesh, in_specs=in_specs, out_specs=out_specs, check_vma=False)
```

```python
import functools
import math
import jax
import jax.numpy as jnp
from jax import lax
from jax.experimental import pallas as pl
from jax.experimental.pallas import tpu as pltpu
from jax.sharding import PartitionSpec as P

NORM_EPS = 1e-6
F32 = jnp.float32
BF16 = jnp.bfloat16
NN = (((1,), (0,)), ((), ()))
NT = (((1,), (1,)), ((), ()))


def dot(lhs, rhs, dims=NN):
    return lax.dot_general(lhs, rhs, dims, preferred_element_type=F32)


def round_up(num, mult):
    return -(-num // mult) * mult


def stats(tokens):
    avg_val = jnp.mean(tokens, axis=-1, keepdims=True)
    centred = tokens - avg_val
    var_val = jnp.mean(centred * centred, axis=-1, keepdims=True)
    inv_std = lax.rsqrt(var_val + NORM_EPS)
    return centred * inv_std, inv_std


def prologue(tok_ref, cot_ref, mod_ref, hid_ref, hid_trn_ref, dy_ref, base, n_valid, chunk):
    @pl.loop(0, tok_ref.shape[0] // chunk)
    def _(step):
        rows = pl.ds(pl.multiple_of(step * chunk, chunk), chunk)
        dst = pl.ds(pl.multiple_of(base + step * chunk, chunk), chunk)
        normed, _ = stats(tok_ref[rows].astype(F32))
        hid = normed * (1.0 + mod_ref[1:2]) + mod_ref[0:1]
        if n_valid < tok_ref.shape[0]:
            row = step * chunk + lax.broadcasted_iota(jnp.int32, hid.shape, 0)
            hid = jnp.where(row < n_valid, hid, 0.0)
        hid = hid.astype(BF16)
        hid_ref[dst] = hid
        hid_trn_ref[:, dst] = hid.T
        dy_ref[dst] = (cot_ref[rows].astype(F32) * mod_ref[2:3]).astype(BF16)


def epilogue(tok_ref, cot_ref, mod_ref, bias, y_ref, acc_ref, new_ref, grad_ref, sums_ref, base, chunk):
    sums_ref[base:base + 4] = jnp.zeros((4, sums_ref.shape[1]), F32)

    @pl.loop(0, tok_ref.shape[0] // chunk)
    def _(step):
        rows = pl.ds(pl.multiple_of(step * chunk, chunk), chunk)
        tokens, cot = tok_ref[rows].astype(F32), cot_ref[rows].astype(F32)
        gate = mod_ref[2:3]
        y_out = y_ref[rows] + bias
        new_ref[rows] = (tokens + gate * y_out).astype(BF16)
        normed, inv_std = stats(tokens)
        d_hid = acc_ref[rows].astype(BF16).astype(F32)
        d_normed = d_hid * (1.0 + mod_ref[1:2])
        mean_d = jnp.mean(d_normed, axis=-1, keepdims=True)
        mean_dn = jnp.mean(d_normed * normed, axis=-1, keepdims=True)
        grad_ref[rows] = (cot + inv_std * (d_normed - mean_d - normed * mean_dn)).astype(BF16)
        sums_ref[base:base + 1] += jnp.sum(d_hid, axis=0, keepdims=True)
        sums_ref[base + 1:base + 2] += jnp.sum(d_hid * normed, axis=0, keepdims=True)
        sums_ref[base + 2:base + 3] += jnp.sum(cot * y_out, axis=0, keepdims=True)
        sums_ref[base + 3:base + 4] += jnp.sum(cot * gate, axis=0, keepdims=True)


def block_kernel(n_keys, heads, tok_i_ref, cot_i_ref, tok_t_ref, cot_t_ref, mod_ref, bo_ref, wq_ref, wk_ref, wv_ref, bq_ref, bk_ref, bv_ref, gain_ref, wo_ref,
                 hid_trn_ref, dy_ref, o_trn_ref, dp_ref, img_ref, txt_ref, sums_ref, dg_ref, db_ref,
                 hid_ref, tok_ref, cot_ref, y_i_ref, y_t_ref, acc_i_ref, acc_t_ref, hat_ref, inv_ref, nat_ref, trn_ref, v_ref, do_nat_ref, do_trn_ref, dq_ref, dk_ref, dv_ref):
    step_b, step_g = pl.program_id(0), pl.program_id(1)
    n_grp = pl.num_programs(1)
    n_img = tok_ref.shape[0]
    width = wq_ref.shape[2]
    head_dim = width // heads
    att_scale = head_dim ** -0.5
    n_tok = n_img + tok_t_ref.shape[1]
    k_rows = round_up(n_keys, 16)
    k_main = k_rows - 16

    @pl.when(step_g == 0)
    def _():
        tok_ref[...] = tok_i_ref[:, 0, 0].reshape(tok_ref.shape)
        cot_ref[...] = cot_i_ref[:, 0, 0].reshape(cot_ref.shape)
        prologue(tok_ref, cot_ref, mod_ref.at[0, 0], hid_ref, hid_trn_ref.at[0], dy_ref.at[0], 0, n_img, 128)
        prologue(tok_t_ref.at[0], cot_t_ref.at[0], mod_ref.at[0, 1], hid_ref, hid_trn_ref.at[0], dy_ref.at[0], n_img, n_keys - n_img, 128)

    hid_i, hid_t = hid_ref[:n_img], hid_ref[n_img:]
    for idx, (w_ref, b_ref) in enumerate(((wq_ref, bq_ref), (wk_ref, bk_ref), (wv_ref, bv_ref))):
        raw_i = dot(hid_i, w_ref[0]) + b_ref[0:1, :]
        raw_t = dot(hid_t, w_ref[1]) + b_ref[1:2, :]
        if idx == 2:
            v_ref[:n_img] = raw_i.astype(BF16)
            v_ref[n_img:] = raw_t.astype(BF16)
            trn_ref[2, :, :n_img] = raw_i.T.astype(BF16)
            trn_ref[2, :, n_img:] = raw_t.T.astype(BF16)
        else:
            raw = jnp.concatenate([raw_i.T, raw_t.T], axis=1).reshape(heads, head_dim, n_tok)
            inv = lax.rsqrt(jnp.mean(raw * raw, axis=1, keepdims=True) + NORM_EPS)
            hat = (raw * inv).reshape(width, n_tok)
            normed = hat * gain_ref[idx]
            hat_ref[idx] = hat
            inv_ref[idx] = inv
            trn_ref[idx] = normed.astype(BF16)
            nat_ref[idx] = normed.T.astype(BF16)

    do_i = dot(dy_ref[0, :n_img], wo_ref[0], NT)
    do_t = dot(dy_ref[0, n_img:], wo_ref[1], NT)
    do_nat_ref[:n_img] = do_i.astype(BF16)
    do_nat_ref[n_img:] = do_t.astype(BF16)
    do_trn_ref[:, :n_img] = do_i.T.astype(BF16)
    do_trn_ref[:, n_img:] = do_t.T.astype(BF16)
    dk_ref[k_rows:] = jnp.zeros((n_tok - k_rows, width), F32)
    dv_ref[k_rows:] = jnp.zeros((n_tok - k_rows, width), F32)

    exp_scale = att_scale * math.log2(math.e)

    def scores_of(head):
        rows = slice(head * head_dim, (head + 1) * head_dim)
        return dot(nat_ref[1, :k_rows, rows], trn_ref[0, rows, :])

    scores = scores_of(0)
    for head in range(heads):
        rows = slice(head * head_dim, (head + 1) * head_dim)
        k_trn, v_trn = trn_ref[1, rows, :k_rows], trn_ref[2, rows, :k_rows]
        q_nat, v_nat = nat_ref[0, :, rows], v_ref[:k_rows, rows]
        do_trn = do_trn_ref[rows]
        ahead = scores_of(head + 1) if head + 1 < heads else None
        d_prob = dot(v_nat, do_trn)
        tail_row = k_main + lax.broadcasted_iota(jnp.int32, (16, n_tok), 0)
        tail = jnp.where(tail_row < n_keys, scores[k_main:], -jnp.inf)
        scores = jnp.concatenate([scores[:k_main], tail], axis=0)
        peak = jnp.max(scores, axis=0, keepdims=True)
        exps = jnp.exp2((scores - peak) * exp_scale)
        inv_sum = 1.0 / jnp.sum(exps, axis=0, keepdims=True)
        prob_lo = (exps * inv_sum).astype(BF16)
        out_trn = dot(v_trn, prob_lo).astype(BF16)
        o_trn_ref[0, rows] = out_trn
        delta = jnp.sum(out_trn.astype(F32) * do_trn.astype(F32), axis=0, keepdims=True)
        d_score = (exps * inv_sum * (d_prob - delta)).astype(BF16)
        dv_ref[:k_rows, rows] = dot(prob_lo, do_nat_ref[:, rows])
        dk_ref[:k_rows, rows] = dot(d_score, q_nat) * att_scale
        dq_ref[rows] = dot(k_trn, d_score) * att_scale
        scores = ahead

    o_nat = o_trn_ref[0].T

    @pl.when(step_g == 0)
    def _():
        y_i_ref[...] = jnp.zeros_like(y_i_ref)
        y_t_ref[...] = jnp.zeros_like(y_t_ref)
        acc_i_ref[...] = jnp.zeros_like(acc_i_ref)
        acc_t_ref[...] = jnp.zeros_like(acc_t_ref)

    @pl.when((step_g == 0) & (step_b == 0))
    def _():
        dg_ref[...] = jnp.zeros_like(dg_ref)

    y_i_ref[...] += dot(o_nat[:n_img], wo_ref[0])
    y_t_ref[...] += dot(o_nat[n_img:], wo_ref[1])

    d_raw = []
    for idx in range(2):
        d_out = dq_ref[...] if idx == 0 else dk_ref[...].T
        d_out = d_out.astype(BF16).astype(F32)
        hat = hat_ref[idx]
        prod = d_out * hat
        dg_ref[idx] += sum(prod[:, lo:lo + 128] for lo in range(0, n_img, 128))
        dg_ref[2 + idx] += sum(prod[:, lo:lo + 128] for lo in range(n_img, n_tok, 128))
        d_hat = (d_out * gain_ref[idx]).reshape(heads, head_dim, n_tok)
        hat = hat.reshape(heads, head_dim, n_tok)
        mean_dh = jnp.mean(d_hat * hat, axis=1, keepdims=True)
        d_raw.append((inv_ref[idx] * (d_hat - hat * mean_dh)).reshape(width, n_tok).T)
    d_raw.append(dv_ref[...].astype(BF16).astype(F32))
    d_lo = []
    for idx in range(3):
        lo = d_raw[idx].astype(BF16)
        dp_ref[0, idx] = lo
        d_lo.append(lo)
        db_ref[0, idx:idx + 1, :] = jnp.sum(d_raw[idx][:n_img], axis=0, keepdims=True)
        db_ref[0, 3 + idx:4 + idx, :] = jnp.sum(d_raw[idx][n_img:], axis=0, keepdims=True)
    db_ref[0, 6:8, :] = jnp.zeros((2, width), F32)
    w_refs = (wq_ref, wk_ref, wv_ref)
    acc_i_ref[...] += sum(dot(d_lo[idx][:n_img], w_refs[idx][0], NT) for idx in range(3))
    acc_t_ref[...] += sum(dot(d_lo[idx][n_img:], w_refs[idx][1], NT) for idx in range(3))

    @pl.when(step_g == n_grp - 1)
    def _():
        epilogue(tok_ref, cot_ref, mod_ref.at[0, 0], bo_ref[0:1], y_i_ref, acc_i_ref, img_ref.at[0, 0], img_ref.at[0, 1], sums_ref.at[0], 0, 64)
        epilogue(tok_t_ref.at[0], cot_t_ref.at[0], mod_ref.at[0, 1], bo_ref[1:2], y_t_ref, acc_t_ref, txt_ref.at[0, 0], txt_ref.at[0, 1], sums_ref.at[0], 4, 64)


def fused_block(tokens, text, cot_t, mod, b_out, w_qkv, b_qkv, qk_gain, w_out, n_keys, heads):
    n_src, _, n_b, tok_dev, d_model = tokens.shape
    n_img, n_txt = n_src * tok_dev, text.shape[1]
    n_tok = n_img + n_txt
    head_dim = qk_gain.shape[-1]
    width = heads * head_dim
    n_grp = d_model // width
    gain_cols = jnp.tile(qk_gain, (1, 1, heads))
    gain_full = jnp.concatenate([jnp.broadcast_to(gain_cols[0][:, :, None], (2, width, n_img)), jnp.broadcast_to(gain_cols[1][:, :, None], (2, width, n_txt))], axis=2)

    def rows_spec(n_rows, **mode):
        return pl.BlockSpec((1, n_rows, d_model), lambda b, g: (b, 0, 0), **mode)

    def w_spec(idx):
        return pl.BlockSpec((2, d_model, width), lambda b, g: (0, 0, idx * n_grp + g))

    def b_spec(idx):
        return pl.BlockSpec((2, width), lambda b, g: (0, idx * n_grp + g))

    def img_spec(idx):
        return pl.BlockSpec((n_src, 1, 1, tok_dev, d_model), lambda b, g: (0, idx, b, 0, 0), pipeline_mode=pl.Buffered(1))

    once = pl.Buffered(1)
    in_specs = [img_spec(0), img_spec(1), rows_spec(n_txt, pipeline_mode=once), rows_spec(n_txt, pipeline_mode=once), pl.BlockSpec((1, 2, 3, d_model), lambda b, g: (b, 0, 0, 0)), pl.BlockSpec((2, d_model), lambda b, g: (0, 0)), w_spec(0), w_spec(1), w_spec(2), b_spec(0), b_spec(1), b_spec(2),
                pl.BlockSpec((2, width, n_tok), lambda b, g: (0, 0, 0)), pl.BlockSpec((2, width, d_model), lambda b, g: (0, g, 0))]
    out_specs = [pl.BlockSpec((1, d_model, n_tok), lambda b, g: (b, 0, 0)), rows_spec(n_tok), pl.BlockSpec((1, width, n_tok), lambda b, g: (b, g, 0)), pl.BlockSpec((1, 3, n_tok, width), lambda b, g: (b, 0, 0, g)),
                 pl.BlockSpec((1, 2, n_img, d_model), lambda b, g: (b, 0, 0, 0)), pl.BlockSpec((1, 2, n_txt, d_model), lambda b, g: (b, 0, 0, 0)), pl.BlockSpec((1, 8, d_model), lambda b, g: (b, 0, 0)),
                 pl.BlockSpec((4, width, 128), lambda b, g: (0, 0, 0)), pl.BlockSpec((1, 8, width), lambda b, g: (b, 0, g))]
    shape = jax.ShapeDtypeStruct
    out_shape = [shape((n_b, d_model, n_tok), BF16), shape((n_b, n_tok, d_model), BF16), shape((n_b, d_model, n_tok), BF16), shape((n_b, 3, n_tok, d_model), BF16),
                 shape((n_b, 2, n_img, d_model), BF16), shape((n_b, 2, n_txt, d_model), BF16), shape((n_b, 8, d_model), F32), shape((4, width, 128), F32), shape((n_b, 8, d_model), F32)]
    scratch = [pltpu.VMEM((n_tok, d_model), BF16), pltpu.VMEM((n_img, d_model), BF16), pltpu.VMEM((n_img, d_model), BF16),
               pltpu.VMEM((n_img, d_model), F32), pltpu.VMEM((n_txt, d_model), F32), pltpu.VMEM((n_img, d_model), F32), pltpu.VMEM((n_txt, d_model), F32),
               pltpu.VMEM((2, width, n_tok), F32), pltpu.VMEM((2, heads, 1, n_tok), F32),
               pltpu.VMEM((2, n_tok, width), BF16), pltpu.VMEM((3, width, n_tok), BF16), pltpu.VMEM((n_tok, width), BF16),
               pltpu.VMEM((n_tok, width), BF16), pltpu.VMEM((width, n_tok), BF16),
               pltpu.VMEM((width, n_tok), F32), pltpu.VMEM((n_tok, width), F32), pltpu.VMEM((n_tok, width), F32)]
    flops = n_b * n_tok * d_model * d_model * 16 + n_b * d_model * n_tok * n_tok * 12
    return pl.pallas_call(
        functools.partial(block_kernel, n_keys, heads),
        out_shape=out_shape, grid=(n_b, n_grp), in_specs=in_specs, out_specs=out_specs, scratch_shapes=scratch,
        compiler_params=pltpu.CompilerParams(dimension_semantics=("arbitrary", "arbitrary"), vmem_limit_bytes=67043328),
        cost_estimate=pl.CostEstimate(flops=flops, bytes_accessed=100 * 1024 * 1024, transcendentals=0),
        name="fused_block",
    )(tokens, tokens, text, cot_t, mod, b_out, w_qkv, w_qkv, w_qkv, b_qkv, b_qkv, b_qkv, gain_full, w_out)


def wgrad_kernel(n_img, n_b, with_ada, core_ref, *refs):
    lefts, rights, refs = refs[:2 * n_b], refs[2 * n_b:4 * n_b], refs[4 * n_b:]
    if with_ada:
        act_ref, dmod_ref, w_ref, out_ref, dw_ref, dact_ref, trn_i_ref, trn_t_ref, rhs_i_ref, rhs_t_ref = refs
    else:
        out_ref, trn_i_ref, trn_t_ref, rhs_i_ref, rhs_t_ref = refs
    d_model, n_tok = lefts[0].shape[1:]
    n_txt = n_tok - n_img
    core = core_ref[0]

    def place(idx, n_rows):
        pos = core * n_b + idx if idx < n_b else (1 - core) * n_b + idx - n_b
        return pl.ds(pl.multiple_of(pos * n_rows, n_rows), n_rows)

    @pl.when(pl.program_id(0) == 0)
    def _():
        for idx in range(2 * n_b):
            trn_i_ref[:, place(idx, n_img)] = lefts[idx][0, :, :n_img]
            trn_t_ref[:, place(idx, n_txt)] = lefts[idx][0, :, n_img:]
        if with_ada:
            dact_ref[...] = jnp.zeros_like(dact_ref)

    for idx in range(2 * n_b):
        rhs_i_ref[place(idx, n_img)] = rights[idx][0, 0, :n_img]
        rhs_t_ref[place(idx, n_txt)] = rights[idx][0, 0, n_img:]

    chunk = 512
    if with_ada:
        dmods = [dmod_ref[branch, 0].astype(BF16) for branch in range(2)]
        dmods_trn = [dmod_ref[branch, 0].T.astype(BF16) for branch in range(2)]

    @pl.loop(0, d_model // chunk)
    def _(step):
        rows = pl.ds(pl.multiple_of(step * chunk, chunk), chunk)
        out_ref[0, rows] = dot(trn_i_ref[rows], rhs_i_ref[...])
        out_ref[1, rows] = dot(trn_t_ref[rows], rhs_t_ref[...])
        if with_ada:
            for branch in range(2):
                dw_ref[branch, rows] = dot(act_ref[rows], dmods[branch])
                dact_ref[rows] += dot(w_ref[branch, rows], dmods_trn[branch])


def wgrad(core, lefts, rights, n_img, block, ada=None):
    n_b = len(lefts) // 2
    _, d_model, n_tok = lefts[0].shape
    n_c, wide = rights[0].shape[1], rights[0].shape[3]
    per = wide // block
    cols = n_c * wide
    left_spec = pl.BlockSpec((1, d_model, n_tok), lambda j: (0, 0, 0), pipeline_mode=pl.Buffered(1))
    right_spec = pl.BlockSpec((1, 1, n_tok, block), lambda j: (0, j // per, 0, j % per))
    mat_spec = pl.BlockSpec((2, d_model, block), lambda j: (0, 0, j))
    in_specs = [pl.BlockSpec(memory_space=pltpu.SMEM)] + [left_spec] * (2 * n_b) + [right_spec] * (2 * n_b)
    out_shape, out_specs, extra = [jax.ShapeDtypeStruct((2, d_model, cols), F32)], [mat_spec], []
    if ada is not None:
        cond_act, d_mod, w_ada = ada
        n_batch = cond_act.shape[0]
        extra = [jnp.pad(cond_act, ((0, 16 - n_batch), (0, 0))).T, jnp.pad(d_mod, ((0, 0), (0, 0), (0, 16 - n_batch), (0, 0))), w_ada]
        in_specs += [pl.BlockSpec((d_model, 16), lambda j: (0, 0)), pl.BlockSpec((2, 1, 16, block), lambda j: (0, j // per, 0, j % per)), mat_spec]
        out_shape += [jax.ShapeDtypeStruct((2, d_model, cols), F32), jax.ShapeDtypeStruct((d_model, 16), F32)]
        out_specs += [mat_spec, pl.BlockSpec((d_model, 16), lambda j: (0, 0))]
    return pl.pallas_call(
        functools.partial(wgrad_kernel, n_img, n_b, ada is not None),
        out_shape=out_shape, grid=(n_c * per,), in_specs=in_specs, out_specs=out_specs,
        scratch_shapes=[pltpu.VMEM((d_model, 2 * n_b * n_img), BF16), pltpu.VMEM((d_model, 2 * n_b * (n_tok - n_img)), BF16),
                        pltpu.VMEM((2 * n_b * n_img, block), BF16), pltpu.VMEM((2 * n_b * (n_tok - n_img), block), BF16)],
        compiler_params=pltpu.CompilerParams(dimension_semantics=("arbitrary",), vmem_limit_bytes=67043328),
        cost_estimate=pl.CostEstimate(flops=4 * n_b * n_tok * d_model * cols, bytes_accessed=(8 if ada is None else 24) * d_model * cols, transcendentals=0),
    )(core[None], *lefts, *rights, *extra)


def ada_fwd_kernel(act_ref, w_ref, b_ref, out_ref):
    out_ref[0] = dot(act_ref[...], w_ref[0]) + b_ref[pl.ds(pl.program_id(0), 1), :]


def ada_fwd(cond_act, w_ada, b_ada, block):
    n_b, d_model = cond_act.shape
    wide = w_ada.shape[2]
    act = jnp.pad(cond_act, ((0, 16 - n_b), (0, 0)))
    return pl.pallas_call(
        ada_fwd_kernel,
        out_shape=jax.ShapeDtypeStruct((2, 16, wide), F32), grid=(2, wide // block),
        in_specs=[pl.BlockSpec((16, d_model), lambda s, j: (0, 0)), pl.BlockSpec((1, d_model, block), lambda s, j: (s, 0, j)), pl.BlockSpec((2, block), lambda s, j: (0, j))],
        out_specs=pl.BlockSpec((1, 16, block), lambda s, j: (s, 0, j)),
        compiler_params=pltpu.CompilerParams(dimension_semantics=("arbitrary", "arbitrary"), vmem_limit_bytes=40 * 1024 * 1024),
        cost_estimate=pl.CostEstimate(flops=64 * d_model * wide, bytes_accessed=4 * d_model * wide, transcendentals=0),
        name="ada_fwd",
    )(act, w_ada, b_ada)[:, :n_b]


def solution(mesh):
    sp_size = mesh.shape['sp']
    pair = 2
    n_chips = sp_size // pair
    pairs = [(idx, idx + 1 - 2 * (idx % pair)) for idx in range(sp_size)]

    def swap(arr):
        return lax.ppermute(arr, 'sp', pairs)

    def device_fn(image_in, text_in, cond_vec, w_ada, b_ada, w_qkv, b_qkv, qk_gain, w_out, b_out, image_cot, text_cot):
        n_batch, tok_dev, d_model = image_in.shape
        ctx_len = text_in.shape[1]
        n_img = tok_dev * sp_size
        n_own = n_batch // pair
        n_txt = round_up(n_img + ctx_len, 128) - n_img
        me = lax.axis_index('sp')
        core, chip = lax.rem(me, pair), lax.div(me, pair)
        own_lo = core * n_own

        img_pair = jnp.stack([image_in, image_cot]).reshape(2, pair, n_own, 1, tok_dev, d_model)
        tokens = [lax.all_to_all(jnp.concatenate([img_pair[:, :, idx].swapaxes(0, 1)] * n_chips, axis=0), 'sp', 0, 0) for idx in range(n_own)]

        def own(arr, axis=0):
            return lax.dynamic_slice_in_dim(arr, own_lo, n_own, axis)

        def ordered(mine, other, axis=0):
            return jnp.where(core == 0, jnp.concatenate([mine, other], axis), jnp.concatenate([other, mine], axis))

        cond_act = jax.nn.silu(cond_vec.astype(F32)).astype(BF16)
        cond_mod = ada_fwd(cond_act, w_ada, b_ada, 1536)
        own_mod = own(cond_mod, 1).reshape(2, n_own, 3, d_model).swapaxes(0, 1)
        pad_rows = ((0, 0), (0, n_txt - ctx_len), (0, 0))
        text_own, cot_own = jnp.pad(own(text_in), pad_rows), jnp.pad(own(text_cot), pad_rows)

        outs, others = [], []
        for idx in range(n_own):
            one = slice(idx, idx + 1)
            out = list(fused_block(tokens[idx], text_own[one], cot_own[one], own_mod[one], b_out, w_qkv, b_qkv, qk_gain, w_out, n_img + ctx_len, 4))
            out[1] = out[1][:, None]
            other = {}
            for pos_set in ((2, 1), (0, 3), (5,)):
                other.update({pos: swap(out[pos]) for pos in pos_set})
            others.append(other)
            outs.append(out)
        hid_trn, dy, o_trn, dp, txt = [[out[pos] for out in outs] + [other[pos] for other in others] for pos in (0, 1, 2, 3, 5)]

        sums = jnp.concatenate([out[6] for out in outs])
        db = sum(out[8] for out in outs)
        dg = jnp.sum(sum(out[7] for out in outs), -1)
        sums_other = swap(sums)
        sums = ordered(sums, sums_other).swapaxes(0, 1).reshape(2, 4, n_batch, d_model)
        rest = jnp.concatenate([db[0, :6], jnp.pad(dg, ((0, 0), (0, d_model - dg.shape[1])))])
        rest_other = swap(rest)
        rest = rest + rest_other
        d_mod, db_out, db_qkv = sums[:, :3], jnp.sum(sums[:, 3], 1), rest[:6].reshape(2, 3 * d_model)
        d_gain = jnp.sum(rest[6:, :dg.shape[1]].reshape(2, 2, -1, qk_gain.shape[-1]), 2)

        dw_out, = wgrad(core, o_trn, dy, n_img, 256)
        dw_qkv, dw_ada, d_act = wgrad(core, hid_trn, dp, n_img, 512, (cond_act, d_mod, w_ada))
        d_act = d_act.T[:n_batch]
        db_ada = jnp.sum(d_mod, axis=2).reshape(2, 3 * d_model)
        _, pull_act = jax.vjp(jax.nn.silu, cond_vec.astype(F32))
        grad_cond = pull_act(d_act.astype(BF16).astype(F32))[0]

        img_pair = jnp.concatenate([out[4] for out in outs])
        chip_lo = chip * pair * tok_dev
        img_mine = lax.dynamic_slice_in_dim(img_pair, chip_lo + core * tok_dev, tok_dev, 2)
        img_send = lax.dynamic_slice_in_dim(img_pair, chip_lo + (1 - core) * tok_dev, tok_dev, 2)
        img_pair = ordered(img_mine, swap(img_send))
        text_new, grad_text = (ordered(jnp.concatenate([arr[:, pos, :ctx_len] for arr in txt[:n_own]]), jnp.concatenate([arr[:, pos, :ctx_len] for arr in txt[n_own:]])) for pos in range(2))
        return (img_pair[:, 0], text_new, img_pair[:, 1], grad_text, grad_cond, dw_ada, db_ada, dw_qkv, db_qkv, d_gain, dw_out, db_out)

    data_spec = P('dp', 'sp', None)
    batch_spec = P('dp')
    rep_spec = P()
    in_specs = (data_spec, batch_spec, batch_spec, rep_spec, rep_spec, rep_spec, rep_spec, rep_spec, rep_spec, rep_spec, data_spec, batch_spec)
    out_specs = (data_spec, batch_spec, data_spec, batch_spec, batch_spec, batch_spec, batch_spec, batch_spec, batch_spec, batch_spec, batch_spec, batch_spec)

    return jax.shard_map(device_fn, mesh=mesh, in_specs=in_specs, out_specs=out_specs, check_vma=False)
```

```python
import functools
import math
import jax
import jax.numpy as jnp
from jax import lax
from jax.experimental import pallas as pl
from jax.experimental.pallas import tpu as pltpu
from jax.sharding import PartitionSpec as P

NORM_EPS = 1e-6
F32 = jnp.float32
BF16 = jnp.bfloat16
NN = (((1,), (0,)), ((), ()))
NT = (((1,), (1,)), ((), ()))


def dot(lhs, rhs, dims=NN):
    return lax.dot_general(lhs, rhs, dims, preferred_element_type=F32)


def round_up(num, mult):
    return -(-num // mult) * mult


def stats(tokens):
    avg_val = jnp.mean(tokens, axis=-1, keepdims=True)
    centred = tokens - avg_val
    var_val = jnp.mean(centred * centred, axis=-1, keepdims=True)
    inv_std = lax.rsqrt(var_val + NORM_EPS)
    return centred * inv_std, inv_std


def prologue(tok_ref, cot_ref, mod_ref, hid_ref, hid_trn_ref, dy_ref, base, n_valid, chunk):
    @pl.loop(0, tok_ref.shape[0] // chunk)
    def _(step):
        rows = pl.ds(pl.multiple_of(step * chunk, chunk), chunk)
        dst = pl.ds(pl.multiple_of(base + step * chunk, chunk), chunk)
        normed, _ = stats(tok_ref[rows].astype(F32))
        hid = normed * (1.0 + mod_ref[1:2]) + mod_ref[0:1]
        if n_valid < tok_ref.shape[0]:
            row = step * chunk + lax.broadcasted_iota(jnp.int32, hid.shape, 0)
            hid = jnp.where(row < n_valid, hid, 0.0)
        hid = hid.astype(BF16)
        hid_ref[dst] = hid
        hid_trn_ref[:, dst] = hid.T
        dy_ref[dst] = (cot_ref[rows].astype(F32) * mod_ref[2:3]).astype(BF16)


def epilogue(tok_ref, cot_ref, mod_ref, bias, y_ref, acc_ref, new_ref, grad_ref, sums_ref, base, chunk):
    sums_ref[base:base + 4] = jnp.zeros((4, sums_ref.shape[1]), F32)

    @pl.loop(0, tok_ref.shape[0] // chunk)
    def _(step):
        rows = pl.ds(pl.multiple_of(step * chunk, chunk), chunk)
        tokens, cot = tok_ref[rows].astype(F32), cot_ref[rows].astype(F32)
        gate = mod_ref[2:3]
        y_out = y_ref[rows] + bias
        new_ref[rows] = (tokens + gate * y_out).astype(BF16)
        normed, inv_std = stats(tokens)
        d_hid = acc_ref[rows].astype(BF16).astype(F32)
        d_normed = d_hid * (1.0 + mod_ref[1:2])
        mean_d = jnp.mean(d_normed, axis=-1, keepdims=True)
        mean_dn = jnp.mean(d_normed * normed, axis=-1, keepdims=True)
        grad_ref[rows] = (cot + inv_std * (d_normed - mean_d - normed * mean_dn)).astype(BF16)
        sums_ref[base:base + 1] += jnp.sum(d_hid, axis=0, keepdims=True)
        sums_ref[base + 1:base + 2] += jnp.sum(d_hid * normed, axis=0, keepdims=True)
        sums_ref[base + 2:base + 3] += jnp.sum(cot * y_out, axis=0, keepdims=True)
        sums_ref[base + 3:base + 4] += jnp.sum(cot * gate, axis=0, keepdims=True)


def block_kernel(n_keys, heads, tok_i_ref, cot_i_ref, tok_t_ref, cot_t_ref, mod_ref, bo_ref, wq_ref, wk_ref, wv_ref, bq_ref, bk_ref, bv_ref, gain_ref, wo_ref,
                 hid_trn_ref, dy_ref, o_trn_ref, dp_ref, img_ref, txt_ref, sums_ref, dg_ref, db_ref,
                 hid_ref, tok_ref, cot_ref, y_i_ref, y_t_ref, acc_i_ref, acc_t_ref, hat_ref, inv_ref, nat_ref, trn_ref, v_ref, do_nat_ref, do_trn_ref, dq_ref, dk_ref, dv_ref):
    step_b, step_g = pl.program_id(0), pl.program_id(1)
    n_grp = pl.num_programs(1)
    n_img = tok_ref.shape[0]
    width = wq_ref.shape[2]
    head_dim = width // heads
    att_scale = head_dim ** -0.5
    n_tok = n_img + tok_t_ref.shape[1]
    k_rows = round_up(n_keys, 16)
    k_main = k_rows - 16

    @pl.when(step_g == 0)
    def _():
        tok_ref[...] = tok_i_ref[:, 0, 0].reshape(tok_ref.shape)
        cot_ref[...] = cot_i_ref[:, 0, 0].reshape(cot_ref.shape)
        prologue(tok_ref, cot_ref, mod_ref.at[0, 0], hid_ref, hid_trn_ref.at[0], dy_ref.at[0], 0, n_img, 128)
        prologue(tok_t_ref.at[0], cot_t_ref.at[0], mod_ref.at[0, 1], hid_ref, hid_trn_ref.at[0], dy_ref.at[0], n_img, n_keys - n_img, 128)

    hid_i, hid_t = hid_ref[:n_img], hid_ref[n_img:k_rows]

    def pad_tail(arr):
        return jnp.concatenate([arr, jnp.zeros((n_tok - k_rows, width), F32)], axis=0)

    for idx, (w_ref, b_ref) in enumerate(((wq_ref, bq_ref), (wk_ref, bk_ref), (wv_ref, bv_ref))):
        raw_i = dot(hid_i, w_ref[0]) + b_ref[0:1, :]
        raw_t = pad_tail(dot(hid_t, w_ref[1]) + b_ref[1:2, :])
        if idx == 2:
            v_ref[:n_img] = raw_i.astype(BF16)
            v_ref[n_img:] = raw_t.astype(BF16)
            trn_ref[2, :, :n_img] = raw_i.T.astype(BF16)
            trn_ref[2, :, n_img:] = raw_t.T.astype(BF16)
        else:
            raw = jnp.concatenate([raw_i.T, raw_t.T], axis=1).reshape(heads, head_dim, n_tok)
            inv = lax.rsqrt(jnp.mean(raw * raw, axis=1, keepdims=True) + NORM_EPS)
            hat = (raw * inv).reshape(width, n_tok)
            normed = hat * gain_ref[idx]
            hat_ref[idx] = hat
            inv_ref[idx] = inv
            trn_ref[idx] = normed.astype(BF16)
            nat_ref[idx] = normed.T.astype(BF16)

    do_i = dot(dy_ref[0, :n_img], wo_ref[0], NT)
    do_t = pad_tail(dot(dy_ref[0, n_img:k_rows], wo_ref[1], NT))
    do_nat_ref[:n_img] = do_i.astype(BF16)
    do_nat_ref[n_img:] = do_t.astype(BF16)
    do_trn_ref[:, :n_img] = do_i.T.astype(BF16)
    do_trn_ref[:, n_img:] = do_t.T.astype(BF16)
    dk_ref[k_rows:] = jnp.zeros((n_tok - k_rows, width), F32)
    dv_ref[k_rows:] = jnp.zeros((n_tok - k_rows, width), F32)

    exp_scale = att_scale * math.log2(math.e)
    two = 2 * head_dim

    def diag_cols(arr):
        top = lax.broadcasted_iota(jnp.int32, arr.shape, 0) < head_dim
        zero = jnp.zeros_like(arr)
        return jnp.concatenate([jnp.where(top, arr, zero), jnp.where(top, zero, arr)], axis=1)

    def diag_rows(arr):
        left = lax.broadcasted_iota(jnp.int32, arr.shape, 1) < head_dim
        zero = jnp.zeros_like(arr)
        return jnp.concatenate([jnp.where(left, arr, zero), jnp.where(left, zero, arr)], axis=0)

    def diag_take(arr):
        return jnp.concatenate([arr[:head_dim, :n_tok], arr[head_dim:, n_tok:]], axis=0)

    def scores_of(lo):
        rows = slice(lo, lo + two)
        return dot(nat_ref[1, :k_rows, rows], diag_cols(trn_ref[0, rows, :]))

    ahead = scores_of(0)
    for lo in range(0, width, two):
        rows = slice(lo, lo + two)
        do_trn = do_trn_ref[rows]
        scores = ahead
        d_prob = dot(v_ref[:k_rows, rows], diag_cols(do_trn))
        if lo + two < width:
            ahead = scores_of(lo + two)
        tail_row = k_main + lax.broadcasted_iota(jnp.int32, (16, 2 * n_tok), 0)
        tail = jnp.where(tail_row < n_keys, scores[k_main:], -jnp.inf)
        scores = jnp.concatenate([scores[:k_main], tail], axis=0)
        peak = jnp.max(scores, axis=0, keepdims=True)
        exps = jnp.exp2((scores - peak) * exp_scale)
        inv_sum = 1.0 / jnp.sum(exps, axis=0, keepdims=True)
        prob_lo = (exps * inv_sum).astype(BF16)
        out_trn = diag_take(dot(trn_ref[2, rows, :k_rows], prob_lo)).astype(BF16)
        o_trn_ref[0, rows] = out_trn
        prod = out_trn.astype(F32) * do_trn.astype(F32)
        delta = jnp.concatenate([jnp.sum(prod[:head_dim], axis=0, keepdims=True), jnp.sum(prod[head_dim:], axis=0, keepdims=True)], axis=1)
        d_score = (exps * inv_sum * (d_prob - delta)).astype(BF16)
        dv_ref[:k_rows, rows] = dot(prob_lo, diag_rows(do_nat_ref[:, rows]))
        dk_ref[:k_rows, rows] = dot(d_score, diag_rows(nat_ref[0, :, rows])) * att_scale
        dq_ref[rows] = diag_take(dot(trn_ref[1, rows, :k_rows], d_score)) * att_scale

    o_nat = o_trn_ref[0].T

    @pl.when(step_g == 0)
    def _():
        y_i_ref[...] = jnp.zeros_like(y_i_ref)
        y_t_ref[...] = jnp.zeros_like(y_t_ref)
        acc_i_ref[...] = jnp.zeros_like(acc_i_ref)
        acc_t_ref[...] = jnp.zeros_like(acc_t_ref)

    @pl.when((step_g == 0) & (step_b == 0))
    def _():
        dg_ref[...] = jnp.zeros_like(dg_ref)

    y_i_ref[...] += dot(o_nat[:n_img], wo_ref[0])
    y_t_ref[:k_rows - n_img] += dot(o_nat[n_img:k_rows], wo_ref[1])

    d_raw = []
    for idx in range(2):
        d_out = dq_ref[...] if idx == 0 else dk_ref[...].T
        d_out = d_out.astype(BF16).astype(F32)
        hat = hat_ref[idx]
        prod = d_out * hat
        dg_ref[idx] += sum(prod[:, lo:lo + 128] for lo in range(0, n_img, 128))
        dg_ref[2 + idx] += sum(prod[:, lo:lo + 128] for lo in range(n_img, n_tok, 128))
        d_hat = (d_out * gain_ref[idx]).reshape(heads, head_dim, n_tok)
        hat = hat.reshape(heads, head_dim, n_tok)
        mean_dh = jnp.mean(d_hat * hat, axis=1, keepdims=True)
        d_raw.append((inv_ref[idx] * (d_hat - hat * mean_dh)).reshape(width, n_tok).T)
    d_raw.append(dv_ref[...].astype(BF16).astype(F32))
    d_lo = []
    for idx in range(3):
        lo = d_raw[idx].astype(BF16)
        dp_ref[0, idx] = lo
        d_lo.append(lo)
        db_ref[0, idx:idx + 1, :] = jnp.sum(d_raw[idx][:n_img], axis=0, keepdims=True)
        db_ref[0, 3 + idx:4 + idx, :] = jnp.sum(d_raw[idx][n_img:], axis=0, keepdims=True)
    db_ref[0, 6:8, :] = jnp.zeros((2, width), F32)
    w_refs = (wq_ref, wk_ref, wv_ref)
    acc_i_ref[...] += sum(dot(d_lo[idx][:n_img], w_refs[idx][0], NT) for idx in range(3))
    acc_t_ref[:k_rows - n_img] += sum(dot(d_lo[idx][n_img:k_rows], w_refs[idx][1], NT) for idx in range(3))

    @pl.when(step_g == n_grp - 1)
    def _():
        epilogue(tok_ref, cot_ref, mod_ref.at[0, 0], bo_ref[0:1], y_i_ref, acc_i_ref, img_ref.at[0, 0], img_ref.at[0, 1], sums_ref.at[0], 0, 64)
        epilogue(tok_t_ref.at[0], cot_t_ref.at[0], mod_ref.at[0, 1], bo_ref[1:2], y_t_ref, acc_t_ref, txt_ref.at[0, 0], txt_ref.at[0, 1], sums_ref.at[0], 4, 64)


def fused_block(tokens, text, cot_t, mod, b_out, w_qkv, b_qkv, qk_gain, w_out, n_keys, heads):
    n_src, _, n_b, tok_dev, d_model = tokens.shape
    n_img, n_txt = n_src * tok_dev, text.shape[1]
    n_tok = n_img + n_txt
    head_dim = qk_gain.shape[-1]
    width = heads * head_dim
    n_grp = d_model // width
    gain_cols = jnp.tile(qk_gain, (1, 1, heads))
    gain_full = jnp.concatenate([jnp.broadcast_to(gain_cols[0][:, :, None], (2, width, n_img)), jnp.broadcast_to(gain_cols[1][:, :, None], (2, width, n_txt))], axis=2)

    def rows_spec(n_rows, **mode):
        return pl.BlockSpec((1, n_rows, d_model), lambda b, g: (b, 0, 0), **mode)

    def w_spec(idx):
        return pl.BlockSpec((2, d_model, width), lambda b, g: (0, 0, idx * n_grp + g))

    def b_spec(idx):
        return pl.BlockSpec((2, width), lambda b, g: (0, idx * n_grp + g))

    def img_spec(idx):
        return pl.BlockSpec((n_src, 1, 1, tok_dev, d_model), lambda b, g: (0, idx, b, 0, 0), pipeline_mode=pl.Buffered(1))

    once = pl.Buffered(1)
    in_specs = [img_spec(0), img_spec(1), rows_spec(n_txt, pipeline_mode=once), rows_spec(n_txt, pipeline_mode=once), pl.BlockSpec((1, 2, 3, d_model), lambda b, g: (b, 0, 0, 0)), pl.BlockSpec((2, d_model), lambda b, g: (0, 0)), w_spec(0), w_spec(1), w_spec(2), b_spec(0), b_spec(1), b_spec(2),
                pl.BlockSpec((2, width, n_tok), lambda b, g: (0, 0, 0)), pl.BlockSpec((2, width, d_model), lambda b, g: (0, g, 0))]
    out_specs = [pl.BlockSpec((1, d_model, n_tok), lambda b, g: (b, 0, 0)), rows_spec(n_tok), pl.BlockSpec((1, width, n_tok), lambda b, g: (b, g, 0)), pl.BlockSpec((1, 3, n_tok, width), lambda b, g: (b, 0, 0, g)),
                 pl.BlockSpec((1, 2, n_img, d_model), lambda b, g: (b, 0, 0, 0)), pl.BlockSpec((1, 2, n_txt, d_model), lambda b, g: (b, 0, 0, 0)), pl.BlockSpec((1, 8, d_model), lambda b, g: (b, 0, 0)),
                 pl.BlockSpec((4, width, 128), lambda b, g: (0, 0, 0)), pl.BlockSpec((1, 8, width), lambda b, g: (b, 0, g))]
    shape = jax.ShapeDtypeStruct
    out_shape = [shape((n_b, d_model, n_tok), BF16), shape((n_b, n_tok, d_model), BF16), shape((n_b, d_model, n_tok), BF16), shape((n_b, 3, n_tok, d_model), BF16),
                 shape((n_b, 2, n_img, d_model), BF16), shape((n_b, 2, n_txt, d_model), BF16), shape((n_b, 8, d_model), F32), shape((4, width, 128), F32), shape((n_b, 8, d_model), F32)]
    scratch = [pltpu.VMEM((n_tok, d_model), BF16), pltpu.VMEM((n_img, d_model), BF16), pltpu.VMEM((n_img, d_model), BF16),
               pltpu.VMEM((n_img, d_model), F32), pltpu.VMEM((n_txt, d_model), F32), pltpu.VMEM((n_img, d_model), F32), pltpu.VMEM((n_txt, d_model), F32),
               pltpu.VMEM((2, width, n_tok), F32), pltpu.VMEM((2, heads, 1, n_tok), F32),
               pltpu.VMEM((2, n_tok, width), BF16), pltpu.VMEM((3, width, n_tok), BF16), pltpu.VMEM((n_tok, width), BF16),
               pltpu.VMEM((n_tok, width), BF16), pltpu.VMEM((width, n_tok), BF16),
               pltpu.VMEM((width, n_tok), F32), pltpu.VMEM((n_tok, width), F32), pltpu.VMEM((n_tok, width), F32)]
    flops = n_b * n_tok * d_model * d_model * 16 + n_b * d_model * n_tok * n_tok * 12
    return pl.pallas_call(
        functools.partial(block_kernel, n_keys, heads),
        out_shape=out_shape, grid=(n_b, n_grp), in_specs=in_specs, out_specs=out_specs, scratch_shapes=scratch,
        compiler_params=pltpu.CompilerParams(dimension_semantics=("arbitrary", "arbitrary"), vmem_limit_bytes=67043328),
        cost_estimate=pl.CostEstimate(flops=flops, bytes_accessed=100 * 1024 * 1024, transcendentals=0),
        name="fused_block",
    )(tokens, tokens, text, cot_t, mod, b_out, w_qkv, w_qkv, w_qkv, b_qkv, b_qkv, b_qkv, gain_full, w_out)


def wgrad_kernel(n_img, n_b, with_ada, core_ref, *refs):
    lefts, rights, refs = refs[:2 * n_b], refs[2 * n_b:4 * n_b], refs[4 * n_b:]
    if with_ada:
        act_ref, dmod_ref, w_ref, out_ref, dw_ref, dact_ref, trn_i_ref, trn_t_ref, rhs_i_ref, rhs_t_ref = refs
    else:
        out_ref, trn_i_ref, trn_t_ref, rhs_i_ref, rhs_t_ref = refs
    d_model, n_tok = lefts[0].shape[1:]
    n_txt = n_tok - n_img
    core = core_ref[0]

    def place(idx, n_rows):
        pos = core * n_b + idx if idx < n_b else (1 - core) * n_b + idx - n_b
        return pl.ds(pl.multiple_of(pos * n_rows, n_rows), n_rows)

    @pl.when(pl.program_id(0) == 0)
    def _():
        for idx in range(2 * n_b):
            trn_i_ref[:, place(idx, n_img)] = lefts[idx][0, :, :n_img]
            trn_t_ref[:, place(idx, n_txt)] = lefts[idx][0, :, n_img:]
        if with_ada:
            dact_ref[...] = jnp.zeros_like(dact_ref)

    for idx in range(2 * n_b):
        rhs_i_ref[place(idx, n_img)] = rights[idx][0, 0, :n_img]
        rhs_t_ref[place(idx, n_txt)] = rights[idx][0, 0, n_img:]

    chunk = 512
    if with_ada:
        dmods_trn = [dmod_ref[branch, 0].T.astype(BF16) for branch in range(2)]

    @pl.loop(0, d_model // chunk)
    def _(step):
        rows = pl.ds(pl.multiple_of(step * chunk, chunk), chunk)
        out_ref[0, rows] = dot(trn_i_ref[rows], rhs_i_ref[...])
        out_ref[1, rows] = dot(trn_t_ref[rows], rhs_t_ref[...])
        if with_ada:
            act = act_ref[rows].astype(F32)
            for branch in range(2):
                dw_ref[branch, rows] = sum(act[:, idx:idx + 1] * dmod_ref[branch, 0, idx:idx + 1, :] for idx in range(2 * n_b))
                dact_ref[rows] += dot(w_ref[branch, rows], dmods_trn[branch])


def wgrad(core, lefts, rights, n_img, block, ada=None):
    n_b = len(lefts) // 2
    _, d_model, n_tok = lefts[0].shape
    n_c, wide = rights[0].shape[1], rights[0].shape[3]
    per = wide // block
    cols = n_c * wide
    left_spec = pl.BlockSpec((1, d_model, n_tok), lambda j: (0, 0, 0), pipeline_mode=pl.Buffered(1))
    right_spec = pl.BlockSpec((1, 1, n_tok, block), lambda j: (0, j // per, 0, j % per))
    mat_spec = pl.BlockSpec((2, d_model, block), lambda j: (0, 0, j))
    in_specs = [pl.BlockSpec(memory_space=pltpu.SMEM)] + [left_spec] * (2 * n_b) + [right_spec] * (2 * n_b)
    out_shape, out_specs, extra = [jax.ShapeDtypeStruct((2, d_model, cols), F32)], [mat_spec], []
    if ada is not None:
        cond_act, d_mod, w_ada = ada
        n_batch = cond_act.shape[0]
        extra = [jnp.pad(cond_act, ((0, 16 - n_batch), (0, 0))).T, jnp.pad(d_mod, ((0, 0), (0, 0), (0, 16 - n_batch), (0, 0))), w_ada]
        in_specs += [pl.BlockSpec((d_model, 16), lambda j: (0, 0)), pl.BlockSpec((2, 1, 16, block), lambda j: (0, j // per, 0, j % per)), mat_spec]
        out_shape += [jax.ShapeDtypeStruct((2, d_model, cols), F32), jax.ShapeDtypeStruct((d_model, 16), F32)]
        out_specs += [mat_spec, pl.BlockSpec((d_model, 16), lambda j: (0, 0))]
    return pl.pallas_call(
        functools.partial(wgrad_kernel, n_img, n_b, ada is not None),
        out_shape=out_shape, grid=(n_c * per,), in_specs=in_specs, out_specs=out_specs,
        scratch_shapes=[pltpu.VMEM((d_model, 2 * n_b * n_img), BF16), pltpu.VMEM((d_model, 2 * n_b * (n_tok - n_img)), BF16),
                        pltpu.VMEM((2 * n_b * n_img, block), BF16), pltpu.VMEM((2 * n_b * (n_tok - n_img), block), BF16)],
        compiler_params=pltpu.CompilerParams(dimension_semantics=("arbitrary",), vmem_limit_bytes=67043328),
        cost_estimate=pl.CostEstimate(flops=4 * n_b * n_tok * d_model * cols, bytes_accessed=(8 if ada is None else 24) * d_model * cols, transcendentals=0),
    )(core[None], *lefts, *rights, *extra)


def ada_fwd_kernel(act_ref, w_ref, b_ref, out_ref):
    out_ref[0] = dot(act_ref[...], w_ref[0]) + b_ref[pl.ds(pl.program_id(0), 1), :]


def ada_fwd(cond_act, w_ada, b_ada, block):
    n_b, d_model = cond_act.shape
    wide = w_ada.shape[2]
    act = jnp.pad(cond_act, ((0, 16 - n_b), (0, 0)))
    return pl.pallas_call(
        ada_fwd_kernel,
        out_shape=jax.ShapeDtypeStruct((2, 16, wide), F32), grid=(2, wide // block),
        in_specs=[pl.BlockSpec((16, d_model), lambda s, j: (0, 0)), pl.BlockSpec((1, d_model, block), lambda s, j: (s, 0, j)), pl.BlockSpec((2, block), lambda s, j: (0, j))],
        out_specs=pl.BlockSpec((1, 16, block), lambda s, j: (s, 0, j)),
        compiler_params=pltpu.CompilerParams(dimension_semantics=("arbitrary", "arbitrary"), vmem_limit_bytes=40 * 1024 * 1024),
        cost_estimate=pl.CostEstimate(flops=64 * d_model * wide, bytes_accessed=4 * d_model * wide, transcendentals=0),
        name="ada_fwd",
    )(act, w_ada, b_ada)[:, :n_b]


def solution(mesh):
    sp_size = mesh.shape['sp']
    pair = 2
    n_chips = sp_size // pair
    pairs = [(idx, idx + 1 - 2 * (idx % pair)) for idx in range(sp_size)]

    def swap(arr):
        return lax.ppermute(arr, 'sp', pairs)

    def device_fn(image_in, text_in, cond_vec, w_ada, b_ada, w_qkv, b_qkv, qk_gain, w_out, b_out, image_cot, text_cot):
        n_batch, tok_dev, d_model = image_in.shape
        ctx_len = text_in.shape[1]
        n_img = tok_dev * sp_size
        n_own = n_batch // pair
        n_txt = round_up(n_img + ctx_len, 128) - n_img
        me = lax.axis_index('sp')
        core, chip = lax.rem(me, pair), lax.div(me, pair)
        own_lo = core * n_own

        img_pair = jnp.stack([image_in, image_cot]).reshape(2, pair, n_own, 1, tok_dev, d_model)
        tokens = [lax.all_to_all(jnp.concatenate([img_pair[:, :, idx].swapaxes(0, 1)] * n_chips, axis=0), 'sp', 0, 0) for idx in range(n_own)]

        def own(arr, axis=0):
            return lax.dynamic_slice_in_dim(arr, own_lo, n_own, axis)

        def ordered(mine, other, axis=0):
            return jnp.where(core == 0, jnp.concatenate([mine, other], axis), jnp.concatenate([other, mine], axis))

        cond_act = jax.nn.silu(cond_vec.astype(F32)).astype(BF16)
        cond_mod = ada_fwd(cond_act, w_ada, b_ada, 768)
        own_mod = own(cond_mod, 1).reshape(2, n_own, 3, d_model).swapaxes(0, 1)
        pad_rows = ((0, 0), (0, n_txt - ctx_len), (0, 0))
        text_own, cot_own = jnp.pad(own(text_in), pad_rows), jnp.pad(own(text_cot), pad_rows)

        outs, others = [], []
        for idx in range(n_own):
            one = slice(idx, idx + 1)
            out = list(fused_block(tokens[idx], text_own[one], cot_own[one], own_mod[one], b_out, w_qkv, b_qkv, qk_gain, w_out, n_img + ctx_len, 4))
            out[1] = out[1][:, None]
            other = {}
            for pos_set in ((2, 1), (0, 3), (5,)):
                other.update({pos: swap(out[pos]) for pos in pos_set})
            others.append(other)
            outs.append(out)
        hid_trn, dy, o_trn, dp, txt = [[out[pos] for out in outs] + [other[pos] for other in others] for pos in (0, 1, 2, 3, 5)]

        sums = jnp.concatenate([out[6] for out in outs])
        db = sum(out[8] for out in outs)
        dg = jnp.sum(sum(out[7] for out in outs), -1)
        sums_other = swap(sums)
        sums = ordered(sums, sums_other).swapaxes(0, 1).reshape(2, 4, n_batch, d_model)
        rest = jnp.concatenate([db[0, :6], jnp.pad(dg, ((0, 0), (0, d_model - dg.shape[1])))])
        rest_other = swap(rest)
        rest = rest + rest_other
        d_mod, db_out, db_qkv = sums[:, :3], jnp.sum(sums[:, 3], 1), rest[:6].reshape(2, 3 * d_model)
        d_gain = jnp.sum(rest[6:, :dg.shape[1]].reshape(2, 2, -1, qk_gain.shape[-1]), 2)

        dw_out, = wgrad(core, o_trn, dy, n_img, 512)
        dw_qkv, dw_ada, d_act = wgrad(core, hid_trn, dp, n_img, 512, (cond_act, d_mod, w_ada))
        d_act = d_act.T[:n_batch]
        db_ada = jnp.sum(d_mod, axis=2).reshape(2, 3 * d_model)
        _, pull_act = jax.vjp(jax.nn.silu, cond_vec.astype(F32))
        grad_cond = pull_act(d_act.astype(BF16).astype(F32))[0]

        chip_lo = chip * pair * tok_dev
        img_mine, img_send = (jnp.concatenate([lax.dynamic_slice_in_dim(out[4], chip_lo + pos * tok_dev, tok_dev, 2) for out in outs]) for pos in (core, 1 - core))
        img_pair = ordered(img_mine, swap(img_send))
        txt = ordered(jnp.concatenate(txt[:n_own]), jnp.concatenate(txt[n_own:]))
        text_new, grad_text = txt[:, 0, :ctx_len], txt[:, 1, :ctx_len]
        return (img_pair[:, 0], text_new, img_pair[:, 1], grad_text, grad_cond, dw_ada, db_ada, dw_qkv, db_qkv, d_gain, dw_out, db_out)

    data_spec = P('dp', 'sp', None)
    batch_spec = P('dp')
    rep_spec = P()
    in_specs = (data_spec, batch_spec, batch_spec, rep_spec, rep_spec, rep_spec, rep_spec, rep_spec, rep_spec, rep_spec, data_spec, batch_spec)
    out_specs = (data_spec, batch_spec, data_spec, batch_spec, batch_spec, batch_spec, batch_spec, batch_spec, batch_spec, batch_spec, batch_spec, batch_spec)

    return jax.shard_map(device_fn, mesh=mesh, in_specs=in_specs, out_specs=out_specs, check_vma=False)
```

```python
import functools
import math
import jax
import jax.numpy as jnp
from jax import lax
from jax.experimental import pallas as pl
from jax.experimental.pallas import tpu as pltpu
from jax.sharding import PartitionSpec as P

NORM_EPS = 1e-6
F32 = jnp.float32
BF16 = jnp.bfloat16
NN = (((1,), (0,)), ((), ()))
NT = (((1,), (1,)), ((), ()))


def dot(lhs, rhs, dims=NN):
    return lax.dot_general(lhs, rhs, dims, preferred_element_type=F32)


def round_up(num, mult):
    return -(-num // mult) * mult


def stats(tokens):
    avg_val = jnp.mean(tokens, axis=-1, keepdims=True)
    centred = tokens - avg_val
    var_val = jnp.mean(centred * centred, axis=-1, keepdims=True)
    inv_std = lax.rsqrt(var_val + NORM_EPS)
    return centred * inv_std, inv_std


def prologue(tok_ref, cot_ref, mod_ref, hid_ref, hid_trn_ref, dy_ref, base, n_valid, chunk):
    @pl.loop(0, tok_ref.shape[0] // chunk)
    def _(step):
        rows = pl.ds(pl.multiple_of(step * chunk, chunk), chunk)
        dst = pl.ds(pl.multiple_of(base + step * chunk, chunk), chunk)
        normed, _ = stats(tok_ref[rows].astype(F32))
        hid = normed * (1.0 + mod_ref[1:2]) + mod_ref[0:1]
        if n_valid < tok_ref.shape[0]:
            row = step * chunk + lax.broadcasted_iota(jnp.int32, hid.shape, 0)
            hid = jnp.where(row < n_valid, hid, 0.0)
        hid = hid.astype(BF16)
        hid_ref[dst] = hid
        hid_trn_ref[:, dst] = hid.T
        dy_ref[dst] = (cot_ref[rows].astype(F32) * mod_ref[2:3]).astype(BF16)


def epilogue(tok_ref, cot_ref, mod_ref, bias, y_ref, acc_ref, new_ref, grad_ref, sums_ref, base, chunk):
    sums_ref[base:base + 4] = jnp.zeros((4, sums_ref.shape[1]), F32)

    @pl.loop(0, tok_ref.shape[0] // chunk)
    def _(step):
        rows = pl.ds(pl.multiple_of(step * chunk, chunk), chunk)
        tokens, cot = tok_ref[rows].astype(F32), cot_ref[rows].astype(F32)
        gate = mod_ref[2:3]
        y_out = y_ref[rows] + bias
        new_ref[rows] = (tokens + gate * y_out).astype(BF16)
        normed, inv_std = stats(tokens)
        d_hid = acc_ref[rows].astype(BF16).astype(F32)
        d_normed = d_hid * (1.0 + mod_ref[1:2])
        mean_d = jnp.mean(d_normed, axis=-1, keepdims=True)
        mean_dn = jnp.mean(d_normed * normed, axis=-1, keepdims=True)
        grad_ref[rows] = (cot + inv_std * (d_normed - mean_d - normed * mean_dn)).astype(BF16)
        sums_ref[base:base + 1] += jnp.sum(d_hid, axis=0, keepdims=True)
        sums_ref[base + 1:base + 2] += jnp.sum(d_hid * normed, axis=0, keepdims=True)
        sums_ref[base + 2:base + 3] += jnp.sum(cot * y_out, axis=0, keepdims=True)
        sums_ref[base + 3:base + 4] += jnp.sum(cot * gate, axis=0, keepdims=True)


def block_kernel(n_keys, heads, tok_i_ref, cot_i_ref, tok_t_ref, cot_t_ref, mod_ref, bo_ref, wq_ref, wk_ref, wv_ref, bq_ref, bk_ref, bv_ref, gain_ref, wo_ref,
                 hid_trn_ref, dy_ref, o_trn_ref, dp_ref, img_ref, txt_ref, sums_ref, dg_ref, db_ref,
                 hid_ref, tok_ref, cot_ref, y_i_ref, y_t_ref, acc_i_ref, acc_t_ref, hat_ref, inv_ref, nat_ref, trn_ref, v_ref, do_nat_ref, do_trn_ref, dq_ref, dk_ref, dv_ref):
    step_b, step_g = pl.program_id(0), pl.program_id(1)
    n_grp = pl.num_programs(1)
    n_img = tok_ref.shape[0]
    width = wq_ref.shape[2]
    head_dim = width // heads
    att_scale = head_dim ** -0.5
    n_tok = n_img + tok_t_ref.shape[1]
    k_rows = round_up(n_keys, 16)
    k_main = k_rows - 16

    @pl.when(step_g == 0)
    def _():
        tok_ref[...] = tok_i_ref[:, 0, 0].reshape(tok_ref.shape)
        cot_ref[...] = cot_i_ref[:, 0, 0].reshape(cot_ref.shape)
        prologue(tok_ref, cot_ref, mod_ref.at[0, 0], hid_ref, hid_trn_ref.at[0], dy_ref.at[0], 0, n_img, 128)
        prologue(tok_t_ref.at[0], cot_t_ref.at[0], mod_ref.at[0, 1], hid_ref, hid_trn_ref.at[0], dy_ref.at[0], n_img, n_keys - n_img, 128)

    hid_i, hid_t = hid_ref[:n_img], hid_ref[n_img:k_rows]

    def pad_tail(arr):
        return jnp.concatenate([arr, jnp.zeros((n_tok - k_rows, width), F32)], axis=0)

    for idx, (w_ref, b_ref) in enumerate(((wq_ref, bq_ref), (wk_ref, bk_ref), (wv_ref, bv_ref))):
        raw_i = dot(hid_i, w_ref[0]) + b_ref[0:1, :]
        raw_t = pad_tail(dot(hid_t, w_ref[1]) + b_ref[1:2, :])
        if idx == 2:
            v_ref[:n_img] = raw_i.astype(BF16)
            v_ref[n_img:] = raw_t.astype(BF16)
            trn_ref[2, :, :n_img] = raw_i.T.astype(BF16)
            trn_ref[2, :, n_img:] = raw_t.T.astype(BF16)
        else:
            raw = jnp.concatenate([raw_i.T, raw_t.T], axis=1).reshape(heads, head_dim, n_tok)
            inv = lax.rsqrt(jnp.mean(raw * raw, axis=1, keepdims=True) + NORM_EPS)
            hat = (raw * inv).reshape(width, n_tok)
            normed = hat * gain_ref[idx]
            hat_ref[idx] = hat
            inv_ref[idx] = inv
            trn_ref[idx] = normed.astype(BF16)
            nat_ref[idx] = normed.T.astype(BF16)

    do_i = dot(dy_ref[0, :n_img], wo_ref[0], NT)
    do_t = pad_tail(dot(dy_ref[0, n_img:k_rows], wo_ref[1], NT))
    do_nat_ref[:n_img] = do_i.astype(BF16)
    do_nat_ref[n_img:] = do_t.astype(BF16)
    do_trn_ref[:, :n_img] = do_i.T.astype(BF16)
    do_trn_ref[:, n_img:] = do_t.T.astype(BF16)
    dk_ref[k_rows:] = jnp.zeros((n_tok - k_rows, width), F32)
    dv_ref[k_rows:] = jnp.zeros((n_tok - k_rows, width), F32)

    exp_scale = att_scale * math.log2(math.e)
    two = 2 * head_dim

    def diag_cols(arr):
        top = lax.broadcasted_iota(jnp.int32, arr.shape, 0) < head_dim
        zero = jnp.zeros_like(arr)
        return jnp.concatenate([jnp.where(top, arr, zero), jnp.where(top, zero, arr)], axis=1)

    def diag_rows(arr):
        left = lax.broadcasted_iota(jnp.int32, arr.shape, 1) < head_dim
        zero = jnp.zeros_like(arr)
        return jnp.concatenate([jnp.where(left, arr, zero), jnp.where(left, zero, arr)], axis=0)

    def diag_take(arr):
        return jnp.concatenate([arr[:head_dim, :n_tok], arr[head_dim:, n_tok:]], axis=0)

    def scores_of(lo):
        rows = slice(lo, lo + two)
        return dot(nat_ref[1, :k_rows, rows], diag_cols(trn_ref[0, rows, :]))

    ahead = scores_of(0)
    for lo in range(0, width, two):
        rows = slice(lo, lo + two)
        do_trn = do_trn_ref[rows]
        scores = ahead
        d_prob = dot(v_ref[:k_rows, rows], diag_cols(do_trn))
        if lo + two < width:
            ahead = scores_of(lo + two)
        tail_row = k_main + lax.broadcasted_iota(jnp.int32, (16, 2 * n_tok), 0)
        tail = jnp.where(tail_row < n_keys, scores[k_main:], -jnp.inf)
        scores = jnp.concatenate([scores[:k_main], tail], axis=0)
        peak = jnp.max(scores, axis=0, keepdims=True)
        exps = jnp.exp2((scores - peak) * exp_scale)
        inv_sum = 1.0 / jnp.sum(exps, axis=0, keepdims=True)
        prob_lo = (exps * inv_sum).astype(BF16)
        out_trn = diag_take(dot(trn_ref[2, rows, :k_rows], prob_lo)).astype(BF16)
        o_trn_ref[0, rows] = out_trn
        prod = out_trn.astype(F32) * do_trn.astype(F32)
        delta = jnp.concatenate([jnp.sum(prod[:head_dim], axis=0, keepdims=True), jnp.sum(prod[head_dim:], axis=0, keepdims=True)], axis=1)
        d_score = (exps * inv_sum * (d_prob - delta)).astype(BF16)
        dv_ref[:k_rows, rows] = dot(prob_lo, diag_rows(do_nat_ref[:, rows]))
        dk_ref[:k_rows, rows] = dot(d_score, diag_rows(nat_ref[0, :, rows])) * att_scale
        dq_ref[rows] = diag_take(dot(trn_ref[1, rows, :k_rows], d_score)) * att_scale

    o_nat = o_trn_ref[0].T

    @pl.when(step_g == 0)
    def _():
        y_i_ref[...] = jnp.zeros_like(y_i_ref)
        y_t_ref[...] = jnp.zeros_like(y_t_ref)
        acc_i_ref[...] = jnp.zeros_like(acc_i_ref)
        acc_t_ref[...] = jnp.zeros_like(acc_t_ref)

    @pl.when((step_g == 0) & (step_b == 0))
    def _():
        dg_ref[...] = jnp.zeros_like(dg_ref)

    y_i_ref[...] += dot(o_nat[:n_img], wo_ref[0])
    y_t_ref[:k_rows - n_img] += dot(o_nat[n_img:k_rows], wo_ref[1])

    d_raw = []
    for idx in range(2):
        d_out = dq_ref[...] if idx == 0 else dk_ref[...].T
        d_out = d_out.astype(BF16).astype(F32)
        hat = hat_ref[idx]
        prod = d_out * hat
        dg_ref[idx] += sum(prod[:, lo:lo + 128] for lo in range(0, n_img, 128))
        dg_ref[2 + idx] += sum(prod[:, lo:lo + 128] for lo in range(n_img, n_tok, 128))
        d_hat = (d_out * gain_ref[idx]).reshape(heads, head_dim, n_tok)
        hat = hat.reshape(heads, head_dim, n_tok)
        mean_dh = jnp.mean(d_hat * hat, axis=1, keepdims=True)
        d_raw.append((inv_ref[idx] * (d_hat - hat * mean_dh)).reshape(width, n_tok).T)
    d_raw.append(dv_ref[...].astype(BF16).astype(F32))
    d_lo = []
    for idx in range(3):
        lo = d_raw[idx].astype(BF16)
        dp_ref[0, idx] = lo
        d_lo.append(lo)
        db_ref[0, idx:idx + 1, :] = jnp.sum(d_raw[idx][:n_img], axis=0, keepdims=True)
        db_ref[0, 3 + idx:4 + idx, :] = jnp.sum(d_raw[idx][n_img:], axis=0, keepdims=True)
    db_ref[0, 6:8, :] = jnp.zeros((2, width), F32)
    w_refs = (wq_ref, wk_ref, wv_ref)
    acc_i_ref[...] += sum(dot(d_lo[idx][:n_img], w_refs[idx][0], NT) for idx in range(3))
    acc_t_ref[:k_rows - n_img] += sum(dot(d_lo[idx][n_img:k_rows], w_refs[idx][1], NT) for idx in range(3))

    @pl.when(step_g == n_grp - 1)
    def _():
        epilogue(tok_ref, cot_ref, mod_ref.at[0, 0], bo_ref[0:1], y_i_ref, acc_i_ref, img_ref.at[0, 0], img_ref.at[0, 1], sums_ref.at[0], 0, 64)
        epilogue(tok_t_ref.at[0], cot_t_ref.at[0], mod_ref.at[0, 1], bo_ref[1:2], y_t_ref, acc_t_ref, txt_ref.at[0, 0], txt_ref.at[0, 1], sums_ref.at[0], 4, 64)


def fused_block(tokens, text, cot_t, mod, b_out, w_qkv, b_qkv, qk_gain, w_out, n_keys, heads):
    n_src, _, n_b, tok_dev, d_model = tokens.shape
    n_img, n_txt = n_src * tok_dev, text.shape[1]
    n_tok = n_img + n_txt
    head_dim = qk_gain.shape[-1]
    width = heads * head_dim
    n_grp = d_model // width
    gain_cols = jnp.tile(qk_gain, (1, 1, heads))
    gain_full = jnp.concatenate([jnp.broadcast_to(gain_cols[0][:, :, None], (2, width, n_img)), jnp.broadcast_to(gain_cols[1][:, :, None], (2, width, n_txt))], axis=2)

    def rows_spec(n_rows, **mode):
        return pl.BlockSpec((1, n_rows, d_model), lambda b, g: (b, 0, 0), **mode)

    def w_spec(idx):
        return pl.BlockSpec((2, d_model, width), lambda b, g: (0, 0, idx * n_grp + g))

    def b_spec(idx):
        return pl.BlockSpec((2, width), lambda b, g: (0, idx * n_grp + g))

    def img_spec(idx):
        return pl.BlockSpec((n_src, 1, 1, tok_dev, d_model), lambda b, g: (0, idx, b, 0, 0), pipeline_mode=pl.Buffered(1))

    once = pl.Buffered(1)
    in_specs = [img_spec(0), img_spec(1), rows_spec(n_txt, pipeline_mode=once), rows_spec(n_txt, pipeline_mode=once), pl.BlockSpec((1, 2, 3, d_model), lambda b, g: (b, 0, 0, 0)), pl.BlockSpec((2, d_model), lambda b, g: (0, 0)), w_spec(0), w_spec(1), w_spec(2), b_spec(0), b_spec(1), b_spec(2),
                pl.BlockSpec((2, width, n_tok), lambda b, g: (0, 0, 0)), pl.BlockSpec((2, width, d_model), lambda b, g: (0, g, 0))]
    out_specs = [pl.BlockSpec((1, d_model, n_tok), lambda b, g: (b, 0, 0)), rows_spec(n_tok), pl.BlockSpec((1, width, n_tok), lambda b, g: (b, g, 0)), pl.BlockSpec((1, 3, n_tok, width), lambda b, g: (b, 0, 0, g)),
                 pl.BlockSpec((1, 2, n_img, d_model), lambda b, g: (b, 0, 0, 0)), pl.BlockSpec((1, 2, n_txt, d_model), lambda b, g: (b, 0, 0, 0)), pl.BlockSpec((1, 8, d_model), lambda b, g: (b, 0, 0)),
                 pl.BlockSpec((4, width, 128), lambda b, g: (0, 0, 0)), pl.BlockSpec((1, 8, width), lambda b, g: (b, 0, g))]
    shape = jax.ShapeDtypeStruct
    out_shape = [shape((n_b, d_model, n_tok), BF16), shape((n_b, n_tok, d_model), BF16), shape((n_b, d_model, n_tok), BF16), shape((n_b, 3, n_tok, d_model), BF16),
                 shape((n_b, 2, n_img, d_model), BF16), shape((n_b, 2, n_txt, d_model), BF16), shape((n_b, 8, d_model), F32), shape((4, width, 128), F32), shape((n_b, 8, d_model), F32)]
    scratch = [pltpu.VMEM((n_tok, d_model), BF16), pltpu.VMEM((n_img, d_model), BF16), pltpu.VMEM((n_img, d_model), BF16),
               pltpu.VMEM((n_img, d_model), F32), pltpu.VMEM((n_txt, d_model), F32), pltpu.VMEM((n_img, d_model), F32), pltpu.VMEM((n_txt, d_model), F32),
               pltpu.VMEM((2, width, n_tok), F32), pltpu.VMEM((2, heads, 1, n_tok), F32),
               pltpu.VMEM((2, n_tok, width), BF16), pltpu.VMEM((3, width, n_tok), BF16), pltpu.VMEM((n_tok, width), BF16),
               pltpu.VMEM((n_tok, width), BF16), pltpu.VMEM((width, n_tok), BF16),
               pltpu.VMEM((width, n_tok), F32), pltpu.VMEM((n_tok, width), F32), pltpu.VMEM((n_tok, width), F32)]
    flops = n_b * n_tok * d_model * d_model * 16 + n_b * d_model * n_tok * n_tok * 12
    return pl.pallas_call(
        functools.partial(block_kernel, n_keys, heads),
        out_shape=out_shape, grid=(n_b, n_grp), in_specs=in_specs, out_specs=out_specs, scratch_shapes=scratch,
        compiler_params=pltpu.CompilerParams(dimension_semantics=("arbitrary", "arbitrary"), vmem_limit_bytes=67043328),
        cost_estimate=pl.CostEstimate(flops=flops, bytes_accessed=100 * 1024 * 1024, transcendentals=0),
        name="fused_block",
    )(tokens, tokens, text, cot_t, mod, b_out, w_qkv, w_qkv, w_qkv, b_qkv, b_qkv, b_qkv, gain_full, w_out)


def wgrad_kernel(n_img, n_b, with_ada, core_ref, *refs):
    lefts, rights, refs = refs[:2 * n_b], refs[2 * n_b:4 * n_b], refs[4 * n_b:]
    if with_ada:
        act_ref, dmod_ref, w_ref, out_ref, dw_ref, dact_ref, trn_i_ref, trn_t_ref, rhs_i_ref, rhs_t_ref = refs
    else:
        out_ref, trn_i_ref, trn_t_ref, rhs_i_ref, rhs_t_ref = refs
    d_model, n_tok = lefts[0].shape[1:]
    n_txt = n_tok - n_img
    core = core_ref[0]

    def place(idx, n_rows):
        pos = core * n_b + idx if idx < n_b else (1 - core) * n_b + idx - n_b
        return pl.ds(pl.multiple_of(pos * n_rows, n_rows), n_rows)

    @pl.when(pl.program_id(0) == 0)
    def _():
        for idx in range(2 * n_b):
            trn_i_ref[:, place(idx, n_img)] = lefts[idx][0, :, :n_img]
            trn_t_ref[:, place(idx, n_txt)] = lefts[idx][0, :, n_img:]
        if with_ada:
            dact_ref[...] = jnp.zeros_like(dact_ref)

    for idx in range(2 * n_b):
        rhs_i_ref[place(idx, n_img)] = rights[idx][0, 0, :n_img]
        rhs_t_ref[place(idx, n_txt)] = rights[idx][0, 0, n_img:]

    chunk = 512
    if with_ada:
        dmods = [dmod_ref[branch, 0].astype(BF16) for branch in range(2)]
        dmods_trn = [dmod_ref[branch, 0].T.astype(BF16) for branch in range(2)]

    @pl.loop(0, d_model // chunk)
    def _(step):
        rows = pl.ds(pl.multiple_of(step * chunk, chunk), chunk)
        out_ref[0, rows] = dot(trn_i_ref[rows], rhs_i_ref[...])
        out_ref[1, rows] = dot(trn_t_ref[rows], rhs_t_ref[...])
        if with_ada:
            for branch in range(2):
                dw_ref[branch, rows] = dot(act_ref[rows], dmods[branch])
                dact_ref[rows] += dot(w_ref[branch, rows], dmods_trn[branch])


def wgrad(core, lefts, rights, n_img, block, ada=None):
    n_b = len(lefts) // 2
    _, d_model, n_tok = lefts[0].shape
    n_c, wide = rights[0].shape[1], rights[0].shape[3]
    per = wide // block
    cols = n_c * wide
    left_spec = pl.BlockSpec((1, d_model, n_tok), lambda j: (0, 0, 0), pipeline_mode=pl.Buffered(1))
    right_spec = pl.BlockSpec((1, 1, n_tok, block), lambda j: (0, j // per, 0, j % per))
    mat_spec = pl.BlockSpec((2, d_model, block), lambda j: (0, 0, j))
    in_specs = [pl.BlockSpec(memory_space=pltpu.SMEM)] + [left_spec] * (2 * n_b) + [right_spec] * (2 * n_b)
    out_shape, out_specs, extra = [jax.ShapeDtypeStruct((2, d_model, cols), F32)], [mat_spec], []
    if ada is not None:
        cond_act, d_mod, w_ada = ada
        n_batch = cond_act.shape[0]
        extra = [jnp.pad(cond_act, ((0, 16 - n_batch), (0, 0))).T, jnp.pad(d_mod, ((0, 0), (0, 0), (0, 16 - n_batch), (0, 0))), w_ada]
        in_specs += [pl.BlockSpec((d_model, 16), lambda j: (0, 0)), pl.BlockSpec((2, 1, 16, block), lambda j: (0, j // per, 0, j % per)), mat_spec]
        out_shape += [jax.ShapeDtypeStruct((2, d_model, cols), F32), jax.ShapeDtypeStruct((d_model, 16), F32)]
        out_specs += [mat_spec, pl.BlockSpec((d_model, 16), lambda j: (0, 0))]
    return pl.pallas_call(
        functools.partial(wgrad_kernel, n_img, n_b, ada is not None),
        out_shape=out_shape, grid=(n_c * per,), in_specs=in_specs, out_specs=out_specs,
        scratch_shapes=[pltpu.VMEM((d_model, 2 * n_b * n_img), BF16), pltpu.VMEM((d_model, 2 * n_b * (n_tok - n_img)), BF16),
                        pltpu.VMEM((2 * n_b * n_img, block), BF16), pltpu.VMEM((2 * n_b * (n_tok - n_img), block), BF16)],
        compiler_params=pltpu.CompilerParams(dimension_semantics=("arbitrary",), vmem_limit_bytes=67043328),
        cost_estimate=pl.CostEstimate(flops=4 * n_b * n_tok * d_model * cols, bytes_accessed=(8 if ada is None else 24) * d_model * cols, transcendentals=0),
    )(core[None], *lefts, *rights, *extra)


def ada_fwd_kernel(act_ref, w_ref, b_ref, out_ref):
    out_ref[0] = dot(act_ref[...], w_ref[0]) + b_ref[pl.ds(pl.program_id(0), 1), :]


def ada_fwd(cond_act, w_ada, b_ada, block):
    n_b, d_model = cond_act.shape
    wide = w_ada.shape[2]
    act = jnp.pad(cond_act, ((0, 16 - n_b), (0, 0)))
    return pl.pallas_call(
        ada_fwd_kernel,
        out_shape=jax.ShapeDtypeStruct((2, 16, wide), F32), grid=(2, wide // block),
        in_specs=[pl.BlockSpec((16, d_model), lambda s, j: (0, 0)), pl.BlockSpec((1, d_model, block), lambda s, j: (s, 0, j)), pl.BlockSpec((2, block), lambda s, j: (0, j))],
        out_specs=pl.BlockSpec((1, 16, block), lambda s, j: (s, 0, j)),
        compiler_params=pltpu.CompilerParams(dimension_semantics=("arbitrary", "arbitrary"), vmem_limit_bytes=40 * 1024 * 1024),
        cost_estimate=pl.CostEstimate(flops=64 * d_model * wide, bytes_accessed=4 * d_model * wide, transcendentals=0),
        name="ada_fwd",
    )(act, w_ada, b_ada)[:, :n_b]


def solution(mesh):
    sp_size = mesh.shape['sp']
    pair = 2
    n_chips = sp_size // pair
    pairs = [(idx, idx + 1 - 2 * (idx % pair)) for idx in range(sp_size)]

    def swap(arr):
        return lax.ppermute(arr, 'sp', pairs)

    def device_fn(image_in, text_in, cond_vec, w_ada, b_ada, w_qkv, b_qkv, qk_gain, w_out, b_out, image_cot, text_cot):
        n_batch, tok_dev, d_model = image_in.shape
        ctx_len = text_in.shape[1]
        n_img = tok_dev * sp_size
        n_own = n_batch // pair
        n_txt = round_up(n_img + ctx_len, 128) - n_img
        me = lax.axis_index('sp')
        core, chip = lax.rem(me, pair), lax.div(me, pair)
        own_lo = core * n_own

        img_pair = jnp.stack([image_in, image_cot]).reshape(2, pair, n_own, 1, tok_dev, d_model)
        tokens = [lax.all_to_all(jnp.concatenate([img_pair[:, :, idx].swapaxes(0, 1)] * n_chips, axis=0), 'sp', 0, 0) for idx in range(n_own)]

        def own(arr, axis=0):
            return lax.dynamic_slice_in_dim(arr, own_lo, n_own, axis)

        def ordered(mine, other, axis=0):
            return jnp.where(core == 0, jnp.concatenate([mine, other], axis), jnp.concatenate([other, mine], axis))

        cond_act = jax.nn.silu(cond_vec.astype(F32)).astype(BF16)
        cond_mod = ada_fwd(cond_act, w_ada, b_ada, 1536)
        own_mod = own(cond_mod, 1).reshape(2, n_own, 3, d_model).swapaxes(0, 1)
        pad_rows = ((0, 0), (0, n_txt - ctx_len), (0, 0))
        text_own, cot_own = jnp.pad(own(text_in), pad_rows), jnp.pad(own(text_cot), pad_rows)

        outs, others = [], []
        for idx in range(n_own):
            one = slice(idx, idx + 1)
            out = list(fused_block(tokens[idx], text_own[one], cot_own[one], own_mod[one], b_out, w_qkv, b_qkv, qk_gain, w_out, n_img + ctx_len, 4))
            out[1] = out[1][:, None]
            other = {}
            for pos_set in ((2, 1), (0, 3), (5,)):
                other.update({pos: swap(out[pos]) for pos in pos_set})
            others.append(other)
            outs.append(out)
        hid_trn, dy, o_trn, dp, txt = [[out[pos] for out in outs] + [other[pos] for other in others] for pos in (0, 1, 2, 3, 5)]

        sums = jnp.concatenate([out[6] for out in outs])
        db = sum(out[8] for out in outs)
        dg = jnp.sum(sum(out[7] for out in outs), -1)
        sums_other = swap(sums)
        sums = ordered(sums, sums_other).swapaxes(0, 1).reshape(2, 4, n_batch, d_model)
        rest = jnp.concatenate([db[0, :6], jnp.pad(dg, ((0, 0), (0, d_model - dg.shape[1])))])
        rest_other = swap(rest)
        rest = rest + rest_other
        d_mod, db_out, db_qkv = sums[:, :3], jnp.sum(sums[:, 3], 1), rest[:6].reshape(2, 3 * d_model)
        d_gain = jnp.sum(rest[6:, :dg.shape[1]].reshape(2, 2, -1, qk_gain.shape[-1]), 2)

        dw_out, = wgrad(core, o_trn, dy, n_img, 512)
        dw_qkv, dw_ada, d_act = wgrad(core, hid_trn, dp, n_img, 512, (cond_act, d_mod, w_ada))
        d_act = d_act.T[:n_batch]
        db_ada = jnp.sum(d_mod, axis=2).reshape(2, 3 * d_model)
        _, pull_act = jax.vjp(jax.nn.silu, cond_vec.astype(F32))
        grad_cond = pull_act(d_act.astype(BF16).astype(F32))[0]

        chip_lo = chip * pair * tok_dev
        img_mine, img_send = (jnp.concatenate([lax.dynamic_slice_in_dim(out[4], chip_lo + pos * tok_dev, tok_dev, 2) for out in outs]) for pos in (core, 1 - core))
        img_pair = ordered(img_mine, swap(img_send))
        text_new, grad_text = (ordered(jnp.concatenate([arr[:, pos, :ctx_len] for arr in txt[:n_own]]), jnp.concatenate([arr[:, pos, :ctx_len] for arr in txt[n_own:]])) for pos in range(2))
        return (img_pair[:, 0], text_new, img_pair[:, 1], grad_text, grad_cond, dw_ada, db_ada, dw_qkv, db_qkv, d_gain, dw_out, db_out)

    data_spec = P('dp', 'sp', None)
    batch_spec = P('dp')
    rep_spec = P()
    in_specs = (data_spec, batch_spec, batch_spec, rep_spec, rep_spec, rep_spec, rep_spec, rep_spec, rep_spec, rep_spec, data_spec, batch_spec)
    out_specs = (data_spec, batch_spec, data_spec, batch_spec, batch_spec, batch_spec, batch_spec, batch_spec, batch_spec, batch_spec, batch_spec, batch_spec)

    return jax.shard_map(device_fn, mesh=mesh, in_specs=in_specs, out_specs=out_specs, check_vma=False)
```
